32 devices in a mesh: dp: 8 (over z, core), mp: 4 (over y, x).
Axes of the slice: x: 2, y: 2, z: 4, core: 2. Of those that a mesh axis runs over, the one named last changes fastest.
Arguments:
- block_input: bfloat16 [4096, 6144], P('dp', 'mp'), may hold values from -6 to 6
- prenorm_gain: float32 [6144], P('mp'), may hold values from 0.5 to 1.5
- weight: bfloat16 [6144, 3072], P('mp', 'dp'), may hold values from -0.078125 to 0.078125
- query: bfloat16 [4096, 3072], P('dp'), may hold values from -6 to 6
- grad_normed: bfloat16 [4096, 3072], P('dp'), may hold values from -6 to 6
- qk_gain: float32 [128], replicated, may hold values from 0.5 to 1.5
Outputs:
- input_gradient: bfloat16 [4096, 6144], P('dp', 'mp')
- grad_weight: float32 [6144, 3072], P('mp', 'dp')
- prenorm_gain_gradient: float32 [6144], P('mp')
- grad_qk_gain: float32 [128], replicated
The draws below stay inside these ranges and needn't reach their ends.
All inputs are finite; a program needn't handle non-finite values.
Results may differ from the reference program's by a relative error of at most 0.0049.
Values may be sent and summed in bfloat16 or wider, within the bound.
A program may use at most 128 MiB of HBM per device.

```python
import jax
import jax.numpy as jnp
from jax import lax

D = 6144
HEADS = 24
HEAD_DIM = 128
WIDTH = 3072
TOKENS = 4096


def level_of(rng, shape, shards, low, largest):
    gain = 1.0
    for axis_at, blocks in shards:
        steps = jax.random.uniform(jax.random.fold_in(jax.random.fold_in(rng, 6), axis_at), (blocks,), jnp.float32, low / len(shards), largest / len(shards))
        gain = gain * jnp.repeat(jnp.exp(steps), shape[axis_at] // blocks).reshape((-1,) + (1,) * (len(shape) - 1 - axis_at))
    return gain


def centred(rng, dims, width, limit, cuts=(), kind=jnp.bfloat16):
    entries = width * jax.random.normal(rng, dims, jnp.float32)
    if cuts:
        entries = entries * level_of(rng, dims, cuts, -0.22, 0.18)
    return jnp.clip(entries, -limit, limit).astype(kind)


def setup_inputs(seed: int = 0) -> dict:
    splits = jax.random.split(jax.random.key(seed), 7)
    block_input = centred(splits[0], (TOKENS, D), 1.0, 6.0, ((0, 8), (1, 4)))
    prenorm_gain = jnp.clip(1.0 + 0.1 * jax.random.normal(splits[1], (D,), jnp.float32), 0.5, 1.5)
    weight = centred(splits[2], (D, WIDTH), D ** -0.5, 0.078125, ((0, 4), (1, 8)))
    query = centred(splits[3], (TOKENS, WIDTH), 1.0, 6.0, ((0, 8),))
    grad_normed = centred(splits[4], (TOKENS, WIDTH), 1.0, 6.0, ((0, 8),))
    qk_gain = jnp.clip(1.0 + 0.1 * jax.random.normal(splits[5], (HEAD_DIM,), jnp.float32), 0.5, 1.5)
    return {"block_input": block_input, "prenorm_gain": prenorm_gain, "weight": weight, "query": query, "grad_normed": grad_normed, "qk_gain": qk_gain}


EPS = 1e-06

def reference(block_input, prenorm_gain, weight, query, grad_normed, qk_gain):
    input_wide_float = block_input.astype(jnp.float32)
    row_average = lax.optimization_barrier(jnp.mean(input_wide_float, axis=1, keepdims=True))
    variance = lax.optimization_barrier(jnp.mean(input_wide_float * input_wide_float, axis=1, keepdims=True)) - row_average * row_average
    reciprocal_deviation = lax.rsqrt(variance + EPS)
    standardized_input = (input_wide_float - row_average) * reciprocal_deviation
    prenormed_rows = (standardized_input * prenorm_gain).astype(jnp.bfloat16)
    q_float = query.astype(jnp.float32).reshape(TOKENS, HEADS, HEAD_DIM)
    q_mean = lax.optimization_barrier(jnp.mean(q_float, axis=2, keepdims=True))
    q_var = lax.optimization_barrier(jnp.mean(q_float * q_float, axis=2, keepdims=True)) - q_mean * q_mean
    q_inv = lax.rsqrt(q_var + EPS)
    qhat = (q_float - q_mean) * q_inv
    upstream = grad_normed.astype(jnp.float32).reshape(TOKENS, HEADS, HEAD_DIM)
    dqhat = upstream * qk_gain
    grad_query = q_inv * (dqhat - lax.optimization_barrier(jnp.mean(dqhat, axis=2, keepdims=True)) - qhat * lax.optimization_barrier(jnp.mean(dqhat * qhat, axis=2, keepdims=True)))
    grad_query = grad_query.reshape(TOKENS, WIDTH).astype(jnp.bfloat16)
    grad_qk_gain = lax.optimization_barrier(jnp.sum(upstream * qhat, axis=(0, 1)))
    grad_weight = jnp.dot(prenormed_rows.T, grad_query, preferred_element_type=jnp.float32)
    gradient_prenormed_input = jnp.dot(grad_query, weight.T, preferred_element_type=jnp.float32)
    prenorm_gain_gradient = lax.optimization_barrier(jnp.sum(gradient_prenormed_input * standardized_input, axis=0))
    standardized_gradient = gradient_prenormed_input * prenorm_gain
    input_gradient = reciprocal_deviation * (standardized_gradient - lax.optimization_barrier(jnp.mean(standardized_gradient, axis=1, keepdims=True)) - standardized_input * lax.optimization_barrier(jnp.mean(standardized_gradient * standardized_input, axis=1, keepdims=True)))
    return (input_gradient.astype(jnp.bfloat16), grad_weight, prenorm_gain_gradient, grad_qk_gain)
```

```python
import functools
import math

import jax
import jax.numpy as jnp
from jax import lax
from jax.experimental import pallas as pl
from jax.experimental.pallas import tpu as pltpu
from jax.sharding import PartitionSpec as P

D = 6144


EPS = 1e-06


def qk_kernel(query_ref, grad_ref, gain_ref, out_ref, contrib_ref):
    @pl.when(pl.program_id(0) == 0)
    def _():
        contrib_ref[...] = jnp.zeros_like(contrib_ref)

    head_size = gain_ref.shape[1]
    gain = gain_ref[...]
    total = jnp.zeros_like(contrib_ref)
    for head in range(query_ref.shape[1] // head_size):
        columns = pl.ds(head * head_size, head_size)
        q_float = query_ref[:, columns].astype(jnp.float32)
        upstream = grad_ref[:, columns].astype(jnp.float32)
        q_mean = jnp.mean(q_float, axis=1, keepdims=True)
        q_var = jnp.mean(q_float * q_float, axis=1, keepdims=True) - q_mean * q_mean
        q_inv = lax.rsqrt(q_var + EPS)
        qhat = (q_float - q_mean) * q_inv
        dqhat = upstream * gain
        dq_mean = jnp.mean(dqhat, axis=1, keepdims=True)
        dq_cross = jnp.mean(dqhat * qhat, axis=1, keepdims=True)
        out_ref[:, columns] = (q_inv * (dqhat - dq_mean - qhat * dq_cross)).astype(out_ref.dtype)
        product = upstream * qhat
        total += jnp.sum(product.reshape(-1, 8, head_size), axis=0)
    contrib_ref[...] += total


def qk_backward(query, grad_normed, qk_gain):
    rows, width = query.shape
    head_size = qk_gain.shape[0]
    block = min(rows, 64)
    grad_query, contrib = pl.pallas_call(
        qk_kernel,
        grid=(rows // block,),
        in_specs=[
            pl.BlockSpec((block, width), lambda i: (i, 0)),
            pl.BlockSpec((block, width), lambda i: (i, 0)),
            pl.BlockSpec((1, head_size), lambda i: (0, 0)),
        ],
        out_specs=[
            pl.BlockSpec((block, width), lambda i: (i, 0)),
            pl.BlockSpec((8, head_size), lambda i: (0, 0)),
        ],
        out_shape=[
            jax.ShapeDtypeStruct((rows, width), jnp.bfloat16),
            jax.ShapeDtypeStruct((8, head_size), jnp.float32),
        ],
        compiler_params=pltpu.CompilerParams(vmem_limit_bytes=32 * 1024 * 1024),
        cost_estimate=pl.CostEstimate(flops=40 * rows * width, bytes_accessed=6 * rows * width, transcendentals=0),
    )(query, grad_normed, qk_gain.reshape(1, -1))
    return grad_query, jnp.sum(contrib, axis=0)


CORES = 2


def line_move(value, shift, valid):
    chips = lax.axis_size("dp") // CORES
    pairs = [
        (chip * CORES + core, (chip + shift) * CORES + core)
        for chip in range(chips)
        for core in range(CORES)
        if 0 <= chip + shift < chips and valid(chip)
    ]
    return lax.ppermute(value, "dp", pairs)


def partner_swap(value):
    count = lax.axis_size("dp")
    pairs = [(at, at - at % CORES + (at + 1) % CORES) for at in range(count)]
    return lax.ppermute(value, "dp", pairs)


def add_kernel(*refs):
    total = refs[0][...]
    for ref in refs[1:-1]:
        total = total + ref[...].astype(jnp.float32)
    refs[-1][...] = total.astype(jnp.bfloat16)


def add_terms(*terms):
    rows, width = terms[0].shape
    block = math.gcd(rows, 256)
    spec = pl.BlockSpec((block, width), lambda i: (i, 0))
    return pl.pallas_call(
        add_kernel,
        grid=(rows // block,),
        in_specs=[spec] * len(terms),
        out_specs=spec,
        out_shape=jax.ShapeDtypeStruct((rows, width), jnp.bfloat16),
        compiler_params=pltpu.CompilerParams(vmem_limit_bytes=16 * 1024 * 1024),
        cost_estimate=pl.CostEstimate(
            flops=3 * rows * width, bytes_accessed=10 * rows * width, transcendentals=0
        ),
    )(*terms)


def permuted(block_input, prenorm_gain, weight, query, grad_normed, qk_gain):
    chips = lax.axis_size("dp") // CORES
    chip = lax.axis_index("dp") // CORES
    core = lax.axis_index("dp") % CORES
    columns = weight.shape[1]
    pair_columns = columns * CORES

    steps = []
    rightward, leftward = weight, weight
    for step in range(1, chips):
        rightward = line_move(rightward, 1, lambda at: at - step + 1 >= 0)
        leftward = line_move(leftward, -1, lambda at: at + step - 1 < chips)
        steps.append((rightward, leftward))

    input_wide_float = block_input.astype(jnp.float32)
    local_sum = jnp.sum(input_wide_float, axis=1)
    local_square = jnp.sum(input_wide_float * input_wide_float, axis=1)
    total_sum, total_square = lax.psum((local_sum, local_square), "mp")
    row_average = (total_sum / D)[:, None]
    reciprocal_deviation = lax.rsqrt((total_square / D)[:, None] - row_average * row_average + EPS)
    standardized_input = (input_wide_float - row_average) * reciprocal_deviation
    prenormed_rows = (standardized_input * prenorm_gain).astype(jnp.bfloat16)
    grad_query, qk_partial = qk_backward(query, grad_normed, qk_gain)

    def chip_columns(offset):
        first = lax.rem(chip + offset + chips, chips) * pair_columns
        return lax.dynamic_slice_in_dim(grad_query, first, pair_columns, 1)

    order = []
    for step in range(1, chips):
        for offset in ((chips - step) % chips, step):
            if offset not in order:
                order.append(offset)
    order.append(0)
    own, theirs = {}, {}
    for offset in order:
        part = lax.dot_general(
            prenormed_rows,
            chip_columns(offset),
            (((0,), (0,)), ((), ())),
            preferred_element_type=jnp.float32,
        )
        own[offset] = lax.dynamic_slice_in_dim(part, core * columns, columns, 1)
        theirs[offset] = partner_swap(
            lax.dynamic_slice_in_dim(part, (1 - core) * columns, columns, 1).astype(jnp.bfloat16)
        )

    to_right, to_left = None, None
    for step in range(1, chips):
        right_terms = [own[chips - step], theirs[chips - step]]
        left_terms = [own[step], theirs[step]]
        if step > 1:
            right_terms.append(to_right)
            left_terms.append(to_left)
        to_right = line_move(add_terms(*right_terms), 1, lambda at: at < step)
        to_left = line_move(add_terms(*left_terms), -1, lambda at: at >= chips - step)
    grad_weight = own[0] + theirs[0].astype(jnp.float32)
    if chips > 1:
        grad_weight = grad_weight + to_right.astype(jnp.float32) + to_left.astype(jnp.float32)

    def product(block, offset):
        other = partner_swap(block)
        first = jnp.where(core == 0, block, other)
        second = jnp.where(core == 0, other, block)
        return lax.dot_general(
            chip_columns(offset),
            jnp.concatenate([first, second], axis=1),
            (((1,), (1,)), ((), ())),
            preferred_element_type=jnp.float32,
        )

    gradient_prenormed_input = product(weight, 0)
    for step in range(1, chips):
        rightward, leftward = steps[step - 1]
        if 2 * step >= chips:
            from_left = chip >= step
            gradient_prenormed_input += product(
                jnp.where(from_left, rightward, leftward), jnp.where(from_left, -step, step)
            )
        else:
            gradient_prenormed_input += product(rightward, -step)
            gradient_prenormed_input += product(leftward, step)

    standardized_gradient = gradient_prenormed_input * prenorm_gain
    slope_mean, slope_cross = lax.psum(
        (
            jnp.sum(standardized_gradient, axis=1),
            jnp.sum(standardized_gradient * standardized_input, axis=1),
        ),
        "mp",
    )
    average_standardized_gradient = (slope_mean / D)[:, None]
    average_cross_term = (slope_cross / D)[:, None]
    input_gradient = (
        reciprocal_deviation
        * (
            standardized_gradient
            - average_standardized_gradient
            - standardized_input * average_cross_term
        )
    ).astype(jnp.bfloat16)
    prenorm_gain_partial = jnp.sum(gradient_prenormed_input * standardized_input, axis=0)
    prenorm_gain_gradient, grad_qk_gain = lax.psum((prenorm_gain_partial, qk_partial), "dp")
    return (input_gradient, grad_weight, prenorm_gain_gradient, grad_qk_gain)


LANES = 128
MESH = pl.DeviceIdType.MESH


def loop(count, body):
    def step(i, carry):
        body(i)
        return carry

    lax.fori_loop(0, count, step, 0)


def aligned(at, size):
    return pl.ds(pl.multiple_of(at * size, size), size)


def fused_kernel(
    sizes,
    x_ref,
    gain_ref,
    w_ref,
    query_ref,
    grad_ref,
    qk_gain_ref,
    input_grad_ref,
    weight_grad_ref,
    gains_ref,
    x,
    w,
    query,
    grad,
    slots,
    grad_query,
    grad_query_out,
    normed_t,
    product,
    product_in,
    own_grad,
    input_grad,
    average,
    deviation,
    slopes,
    row_sums,
    gain_parts,
    qk_part,
    load_sem,
    store_sem,
    send_sem,
    recv_sem,
    query_sem,
    normed_sem,
    product_sem,
    sums_sem,
    gain_sem,
):
    dp_count, mp_count, pieces = sizes
    chips = dp_count // CORES
    tokens, rows = x_ref.shape
    columns = w_ref.shape[1]
    piece_rows = rows // pieces
    width = rows * mp_count
    blocks, _, block = product.shape
    row_blocks = tokens // LANES
    heads = columns // LANES

    dp = lax.axis_index("dp")
    mp = lax.axis_index("mp")
    chip = dp // CORES
    core = dp % CORES
    partner = (chip * CORES + 1 - core, mp)

    def dp_peer(k):
        return (lax.rem(dp + k, dp_count), mp)

    def mp_peer(k):
        return (dp, lax.rem(mp + k, mp_count))

    loads = [
        pltpu.make_async_copy(source, target, load_sem.at[i])
        for i, (source, target) in enumerate(
            ((x_ref, x), (query_ref, query), (grad_ref, grad), (w_ref, w))
        )
    ]
    for load in loads:
        load.start()

    barrier = pltpu.get_barrier_semaphore()

    def greet(peer):
        pl.semaphore_signal(barrier, inc=1, device_id=peer, device_id_type=MESH)

    loop(dp_count - 1, lambda k: greet(dp_peer(k + 1)))
    loop(mp_count - 1, lambda k: greet(mp_peer(k + 1)))
    pl.semaphore_wait(barrier, dp_count + mp_count - 2)

    def place(way):
        behind = jnp.where(way == 0, chip, chips - 1 - chip)
        return behind, behind < chips - 1

    def hop(way, slot, piece, source):
        part = aligned(piece, piece_rows)
        return pltpu.make_async_remote_copy(
            src_ref=source.at[part],
            dst_ref=slots.at[way, slot, part],
            send_sem=send_sem.at[way, slot, piece],
            recv_sem=recv_sem.at[way, slot, piece],
            device_id=(dp + CORES * (1 - 2 * way), mp),
            device_id_type=MESH,
        )

    def arrival(way, slot, piece):
        return hop(way, slot, piece, slots.at[way, slot])

    def send_weight(piece):
        def one(way):
            @pl.when(place(way)[1])
            def _():
                hop(way, 0, piece, w_ref).start()

        loop(2, one)

    loop(pieces, send_weight)

    def spread(kind, k):
        mine = row_sums.at[kind, mp]
        return pltpu.make_async_remote_copy(
            src_ref=mine,
            dst_ref=mine,
            send_sem=sums_sem.at[kind, 0, k],
            recv_sem=sums_sem.at[kind, 1, k],
            device_id=mp_peer(k),
            device_id_type=MESH,
        )

    diagonal = lax.broadcasted_iota(jnp.int32, (LANES, LANES), 0) == lax.broadcasted_iota(
        jnp.int32, (LANES, LANES), 1
    )

    def as_row(tile):
        total = jnp.sum(tile, axis=1, keepdims=True)
        return jnp.sum(jnp.where(diagonal, total, 0.0), axis=0, keepdims=True)

    def as_tile(row):
        total = jnp.sum(jnp.where(diagonal, row, 0.0), axis=1, keepdims=True)
        return jnp.broadcast_to(total, (LANES, LANES))

    loads[0].wait()

    def input_sums(at):
        part = aligned(at, LANES)
        total = jnp.zeros((LANES, LANES), jnp.float32)
        square = jnp.zeros((LANES, LANES), jnp.float32)
        for k in range(rows // LANES):
            value = x[part, k * LANES : (k + 1) * LANES].astype(jnp.float32)
            total += value
            square += value * value
        row_sums[0, mp, pl.ds(at, 1), :] = as_row(total)
        row_sums[0, mp, pl.ds(row_blocks + at, 1), :] = as_row(square)

    loop(row_blocks, input_sums)
    loop(mp_count - 1, lambda k: spread(0, k + 1).start())

    loads[1].wait()
    loads[2].wait()
    qk_gain = qk_gain_ref[...]
    qk_part[...] = jnp.zeros_like(qk_part)
    chunk = 64

    def qk_columns(to_chip, half, target):
        first = (to_chip * CORES + half) * columns

        def some_rows(at):
            part = aligned(at, chunk)
            total = jnp.zeros_like(qk_part)
            for head in range(heads):
                lanes = pl.ds(pl.multiple_of(first + head * LANES, LANES), LANES)
                q_float = query[part, lanes].astype(jnp.float32)
                upstream = grad[part, lanes].astype(jnp.float32)
                q_mean = jnp.mean(q_float, axis=1, keepdims=True)
                q_var = jnp.mean(q_float * q_float, axis=1, keepdims=True) - q_mean * q_mean
                q_inv = lax.rsqrt(q_var + EPS)
                qhat = (q_float - q_mean) * q_inv
                dqhat = upstream * qk_gain
                dq_mean = jnp.mean(dqhat, axis=1, keepdims=True)
                dq_cross = jnp.mean(dqhat * qhat, axis=1, keepdims=True)
                out = q_inv * (dqhat - dq_mean - qhat * dq_cross)
                target[to_chip, part, head * LANES : (head + 1) * LANES] = out.astype(jnp.bfloat16)
                total += jnp.sum((upstream * qhat).reshape(-1, 8, LANES), axis=0)
            qk_part[...] += total

        loop(tokens // chunk, some_rows)

    def share_query(to_chip):
        return pltpu.make_async_remote_copy(
            src_ref=grad_query_out.at[to_chip],
            dst_ref=grad_query.at[to_chip, pl.ds(tokens, tokens)],
            send_sem=query_sem.at[0, to_chip],
            recv_sem=query_sem.at[1, to_chip],
            device_id=partner,
            device_id_type=MESH,
        )

    def partner_columns(to_chip):
        qk_columns(to_chip, 1 - core, grad_query_out)
        share_query(to_chip).start()

    loop(chips, partner_columns)
    loop(chips, lambda to_chip: qk_columns(to_chip, core, grad_query))

    def gathered(kind):
        total = row_sums[kind, 0]
        for peer in range(1, mp_count):
            total += row_sums[kind, peer]
        return total * (1.0 / width)

    loop(mp_count - 1, lambda k: spread(0, k + 1).wait())
    sums = gathered(0)
    means = sums[:row_blocks]
    scales = lax.rsqrt(sums[row_blocks:] - means * means + EPS)
    for at in range(row_blocks):
        average[at * LANES : (at + 1) * LANES, :] = as_tile(means[at : at + 1])
        deviation[at * LANES : (at + 1) * LANES, :] = as_tile(scales[at : at + 1])

    def standardized(part, lanes):
        return (x[part, lanes].astype(jnp.float32) - average[part, :]) * deviation[part, :]

    def share_normed(piece):
        part = aligned(piece, piece_rows)
        return pltpu.make_async_remote_copy(
            src_ref=normed_t.at[0, part],
            dst_ref=normed_t.at[1, part],
            send_sem=normed_sem.at[0, piece],
            recv_sem=normed_sem.at[1, piece],
            device_id=partner,
            device_id_type=MESH,
        )

    def normalize(piece):
        def some_lanes(k):
            lanes = aligned(piece * (piece_rows // LANES) + k, LANES)
            scale = gain_ref[:, lanes]
            for at in range(row_blocks):
                part = slice(at * LANES, (at + 1) * LANES)
                value = standardized(part, lanes) * scale
                normed_t[0, lanes, part] = value.T.astype(jnp.bfloat16)

        loop(piece_rows // LANES, some_lanes)
        share_normed(piece).start()

    loop(pieces, normalize)

    loop(chips, lambda to_chip: share_query(to_chip).wait_recv())
    loop(pieces, lambda piece: share_normed(piece).wait_recv())

    def contribution(part, to_chip):
        def half(which):
            return jnp.dot(
                normed_t[which, part, :],
                grad_query[to_chip, which * tokens : (which + 1) * tokens, :],
                preferred_element_type=jnp.float32,
            )

        return half(0) + half(1)

    def weight_product(from_chip, weight, first):
        def some_rows(at):
            value = lax.dot_general(
                grad_query[from_chip],
                weight[aligned(at, block), :],
                (((1,), (1,)), ((), ())),
                preferred_element_type=jnp.float32,
            )
            if first:
                product[at] = value
            else:
                product[at] += value

        loop(blocks, some_rows)

    loads[3].wait()

    def slot_step(slot):
        def piece_step(piece):
            part = aligned(piece, piece_rows)

            def take(way):
                behind, ahead = place(way)

                @pl.when(behind > 0)
                def _():
                    arrival(way, slot, piece).wait_recv()

                @pl.when(ahead & (slot >= behind))
                def _():
                    skip = slot - behind
                    to_chip = jnp.where(way == 0, chips - 1 - skip, skip)
                    own = contribution(part, to_chip)

                    @pl.when(behind > 0)
                    def _():
                        held = slots[way, slot, part, :].astype(jnp.float32)
                        slots[way, slot, part, :] = (held + own).astype(jnp.bfloat16)

                    @pl.when(behind == 0)
                    def _():
                        slots[way, slot, part, :] = own.astype(jnp.bfloat16)

            def give(way):
                @pl.when(place(way)[1])
                def _():
                    hop(way, slot + 1, piece, slots.at[way, slot]).start()

            loop(2, take)
            loop(2, give)

        loop(pieces, piece_step)

        @pl.when(slot == 0)
        def _():
            weight_product(chip, w, True)

            def own_piece(piece):
                part = aligned(piece, piece_rows)
                own_grad[part, :] = contribution(part, chip)

            loop(pieces, own_piece)

        def use_weight(way):
            behind, _ = place(way)

            @pl.when(slot < behind)
            def _():
                from_chip = jnp.where(way == 0, chip - 1 - slot, chip + 1 + slot)
                weight_product(from_chip, slots.at[way, slot], False)

        loop(2, use_weight)

    loop(chips - 1, slot_step)

    def share_product(at):
        return pltpu.make_async_remote_copy(
            src_ref=product.at[at, pl.ds(tokens, tokens)],
            dst_ref=product_in.at[at],
            send_sem=product_sem.at[0, at],
            recv_sem=product_sem.at[1, at],
            device_id=partner,
            device_id_type=MESH,
        )

    loop(blocks, lambda at: share_product(at).start())

    slopes[...] = jnp.zeros_like(slopes)
    per_block = block // LANES

    def slope_sums(at):
        share_product(at).wait_recv()
        for k in range(per_block):
            inner = slice(k * LANES, (k + 1) * LANES)
            lanes = aligned(at * per_block + k, LANES)
            scale = gain_ref[:, lanes]

            def some_rows(row, gain_total):
                part = aligned(row, LANES)
                value = product[at, part, inner] + product_in[at, part, inner]
                product[at, part, inner] = value
                xhat = standardized(part, lanes)
                slope = value * scale
                slopes[0, part, :] += slope
                slopes[1, part, :] += slope * xhat
                return gain_total + jnp.sum((value * xhat).reshape(-1, 8, LANES), axis=0)

            gain_total = lax.fori_loop(0, row_blocks, some_rows, jnp.zeros((8, LANES), jnp.float32))
            gain_parts[dp, pl.ds(at * per_block + k, 1), :] = jnp.sum(gain_total, axis=0, keepdims=True)

    loop(blocks, slope_sums)
    for at in range(row_blocks):
        part = slice(at * LANES, (at + 1) * LANES)
        row_sums[1, mp, at : at + 1, :] = as_row(slopes[0, part, :])
        row_sums[1, mp, row_blocks + at : row_blocks + at + 1, :] = as_row(slopes[1, part, :])
    loop(mp_count - 1, lambda k: spread(1, k + 1).start())

    gain_rows = rows // LANES
    padding = gain_parts.shape[1] - gain_rows
    last = lax.broadcasted_iota(jnp.int32, (padding, LANES), 0) == 0
    gain_parts[dp, gain_rows:, :] = jnp.where(last, jnp.sum(qk_part[...], axis=0, keepdims=True), 0.0)

    def share_gains(k):
        mine = gain_parts.at[dp]
        return pltpu.make_async_remote_copy(
            src_ref=mine,
            dst_ref=mine,
            send_sem=gain_sem.at[0, k],
            recv_sem=gain_sem.at[1, k],
            device_id=dp_peer(k),
            device_id_type=MESH,
        )

    loop(dp_count - 1, lambda k: share_gains(k + 1).start())

    loop(mp_count - 1, lambda k: spread(1, k + 1).wait())
    sums = gathered(1)
    for at in range(row_blocks):
        part = slice(at * LANES, (at + 1) * LANES)
        slopes[0, part, :] = as_tile(sums[at : at + 1])
        slopes[1, part, :] = as_tile(sums[row_blocks + at : row_blocks + at + 1])

    def store_input_grad(row):
        part = aligned(row, LANES)
        return pltpu.make_async_copy(input_grad.at[part], input_grad_ref.at[part], store_sem.at[0, row])

    def finish_rows(row):
        part = aligned(row, LANES)
        for k in range(gain_rows):
            lanes = slice(k * LANES, (k + 1) * LANES)
            at, inner = k // per_block, k % per_block * LANES
            slope = product[at, part, inner : inner + LANES] * gain_ref[:, lanes]
            value = deviation[part, :] * (
                slope - slopes[0, part, :] - standardized(part, lanes) * slopes[1, part, :]
            )
            input_grad[part, lanes] = value.astype(jnp.bfloat16)
        store_input_grad(row).start()

    loop(row_blocks, finish_rows)

    loop(dp_count - 1, lambda k: share_gains(k + 1).wait())

    def add_gains(k, total):
        return total + gain_parts[k]

    gains_ref[...] = lax.fori_loop(1, dp_count, add_gains, gain_parts[0])

    def store_weight_grad(piece):
        part = aligned(piece, piece_rows)
        return pltpu.make_async_copy(own_grad.at[part], weight_grad_ref.at[part], store_sem.at[1, piece])

    def finish_piece(piece):
        part = aligned(piece, piece_rows)

        def one(way):
            @pl.when(place(way)[0] > 0)
            def _():
                arrival(way, chips - 1, piece).wait_recv()
                own_grad[part, :] += slots[way, chips - 1, part, :].astype(jnp.float32)

        loop(2, one)
        store_weight_grad(piece).start()

    loop(pieces, finish_piece)

    loop(chips, lambda to_chip: share_query(to_chip).wait_send())
    loop(pieces, lambda piece: share_normed(piece).wait_send())
    loop(blocks, lambda at: share_product(at).wait_send())

    def sent(way):
        @pl.when(place(way)[1])
        def _():
            def of_slot(slot):
                loop(pieces, lambda piece: arrival(way, slot, piece).wait_send())

            loop(chips, of_slot)

    loop(2, sent)
    loop(row_blocks, lambda row: store_input_grad(row).wait())
    loop(pieces, lambda piece: store_weight_grad(piece).wait())


def fused(block_input, prenorm_gain, weight, query, grad_normed, qk_gain):
    dp_count, mp_count = lax.axis_size("dp"), lax.axis_size("mp")
    chips = dp_count // CORES
    tokens, rows = block_input.shape
    columns = weight.shape[1]
    features = query.shape[1]
    pieces = next(count for count in (4, 3, 2, 1) if rows // LANES % count == 0)
    block = math.gcd(rows, 2 * LANES)
    gain_rows = (rows // LANES + 8) // 8 * 8
    anywhere = pl.BlockSpec(memory_space=pl.ANY)
    local = pl.BlockSpec(memory_space=pltpu.VMEM)
    bf16, f32 = jnp.bfloat16, jnp.float32
    dma = pltpu.SemaphoreType.DMA
    input_gradient, grad_weight, gains = pl.pallas_call(
        functools.partial(fused_kernel, (dp_count, mp_count, pieces)),
        in_specs=[anywhere, local, anywhere, anywhere, anywhere, local],
        out_specs=[anywhere, anywhere, local],
        out_shape=[
            jax.ShapeDtypeStruct((tokens, rows), bf16),
            jax.ShapeDtypeStruct((rows, columns), f32),
            jax.ShapeDtypeStruct((gain_rows, LANES), f32),
        ],
        scratch_shapes=[
            pltpu.VMEM((tokens, rows), bf16),
            pltpu.VMEM((rows, columns), bf16),
            pltpu.VMEM((tokens, features), bf16),
            pltpu.VMEM((tokens, features), bf16),
            pltpu.VMEM((2, chips, rows, columns), bf16),
            pltpu.VMEM((chips, CORES * tokens, columns), bf16),
            pltpu.VMEM((chips, tokens, columns), bf16),
            pltpu.VMEM((CORES, rows, tokens), bf16),
            pltpu.VMEM((rows // block, CORES * tokens, block), f32),
            pltpu.VMEM((rows // block, tokens, block), f32),
            pltpu.VMEM((rows, columns), f32),
            pltpu.VMEM((tokens, rows), bf16),
            pltpu.VMEM((tokens, LANES), f32),
            pltpu.VMEM((tokens, LANES), f32),
            pltpu.VMEM((2, tokens, LANES), f32),
            pltpu.VMEM((2, mp_count, 2 * tokens // LANES, LANES), f32),
            pltpu.VMEM((dp_count, gain_rows, LANES), f32),
            pltpu.VMEM((8, LANES), f32),
            dma((4,)),
            dma((2, max(tokens // LANES, pieces))),
            dma((2, chips, pieces)),
            dma((2, chips, pieces)),
            dma((2, chips)),
            dma((2, pieces)),
            dma((2, rows // block)),
            dma((2, 2, mp_count)),
            dma((2, dp_count)),
        ],
        compiler_params=pltpu.CompilerParams(
            collective_id=0, has_side_effects=True, vmem_limit_bytes=56 * 1024 * 1024
        ),
        cost_estimate=pl.CostEstimate(
            flops=8 * tokens * rows * features, bytes_accessed=8 * tokens * features, transcendentals=0
        ),
    )(block_input, prenorm_gain.reshape(1, -1), weight, query, grad_normed, qk_gain.reshape(1, -1))
    count = rows // LANES
    return input_gradient, grad_weight, gains[:count].reshape(-1), gains[count]


def shards(block_input, prenorm_gain, weight, query, grad_normed, qk_gain):
    tokens, rows = block_input.shape
    sizes = (tokens, rows, weight.shape[1])
    whole_tiles = all(size % LANES == 0 for size in sizes) and qk_gain.shape[0] == LANES
    several = lax.axis_size("dp") > CORES and lax.axis_size("mp") > 1
    body = fused if whole_tiles and several else permuted
    return body(block_input, prenorm_gain, weight, query, grad_normed, qk_gain)


def solution(mesh):
    return jax.shard_map(
        shards,
        mesh=mesh,
        in_specs=(P("dp", "mp"), P("mp"), P("mp", "dp"), P("dp", None), P("dp", None), P()),
        out_specs=(P("dp", "mp"), P("mp", "dp"), P("mp"), P()),
        check_vma=False,
    )
```

```python
import functools
import math

import jax
import jax.numpy as jnp
from jax import lax
from jax.experimental import pallas as pl
from jax.experimental.pallas import tpu as pltpu
from jax.sharding import PartitionSpec as P

D = 6144


EPS = 1e-06


def qk_kernel(query_ref, grad_ref, gain_ref, out_ref, contrib_ref):
    @pl.when(pl.program_id(0) == 0)
    def _():
        contrib_ref[...] = jnp.zeros_like(contrib_ref)

    head_size = gain_ref.shape[1]
    gain = gain_ref[...]
    total = jnp.zeros_like(contrib_ref)
    for head in range(query_ref.shape[1] // head_size):
        columns = pl.ds(head * head_size, head_size)
        q_float = query_ref[:, columns].astype(jnp.float32)
        upstream = grad_ref[:, columns].astype(jnp.float32)
        q_mean = jnp.mean(q_float, axis=1, keepdims=True)
        q_var = jnp.mean(q_float * q_float, axis=1, keepdims=True) - q_mean * q_mean
        q_inv = lax.rsqrt(q_var + EPS)
        qhat = (q_float - q_mean) * q_inv
        dqhat = upstream * gain
        dq_mean = jnp.mean(dqhat, axis=1, keepdims=True)
        dq_cross = jnp.mean(dqhat * qhat, axis=1, keepdims=True)
        out_ref[:, columns] = (q_inv * (dqhat - dq_mean - qhat * dq_cross)).astype(out_ref.dtype)
        product = upstream * qhat
        total += jnp.sum(product.reshape(-1, 8, head_size), axis=0)
    contrib_ref[...] += total


def qk_backward(query, grad_normed, qk_gain):
    rows, width = query.shape
    head_size = qk_gain.shape[0]
    block = min(rows, 64)
    grad_query, contrib = pl.pallas_call(
        qk_kernel,
        grid=(rows // block,),
        in_specs=[
            pl.BlockSpec((block, width), lambda i: (i, 0)),
            pl.BlockSpec((block, width), lambda i: (i, 0)),
            pl.BlockSpec((1, head_size), lambda i: (0, 0)),
        ],
        out_specs=[
            pl.BlockSpec((block, width), lambda i: (i, 0)),
            pl.BlockSpec((8, head_size), lambda i: (0, 0)),
        ],
        out_shape=[
            jax.ShapeDtypeStruct((rows, width), jnp.bfloat16),
            jax.ShapeDtypeStruct((8, head_size), jnp.float32),
        ],
        compiler_params=pltpu.CompilerParams(vmem_limit_bytes=32 * 1024 * 1024),
        cost_estimate=pl.CostEstimate(flops=40 * rows * width, bytes_accessed=6 * rows * width, transcendentals=0),
    )(query, grad_normed, qk_gain.reshape(1, -1))
    return grad_query, jnp.sum(contrib, axis=0)


CORES = 2


def line_move(value, shift, valid):
    chips = lax.axis_size("dp") // CORES
    pairs = [
        (chip * CORES + core, (chip + shift) * CORES + core)
        for chip in range(chips)
        for core in range(CORES)
        if 0 <= chip + shift < chips and valid(chip)
    ]
    return lax.ppermute(value, "dp", pairs)


def partner_swap(value):
    count = lax.axis_size("dp")
    pairs = [(at, at - at % CORES + (at + 1) % CORES) for at in range(count)]
    return lax.ppermute(value, "dp", pairs)


def add_kernel(*refs):
    total = refs[0][...]
    for ref in refs[1:-1]:
        total = total + ref[...].astype(jnp.float32)
    refs[-1][...] = total.astype(jnp.bfloat16)


def add_terms(*terms):
    rows, width = terms[0].shape
    block = math.gcd(rows, 256)
    spec = pl.BlockSpec((block, width), lambda i: (i, 0))
    return pl.pallas_call(
        add_kernel,
        grid=(rows // block,),
        in_specs=[spec] * len(terms),
        out_specs=spec,
        out_shape=jax.ShapeDtypeStruct((rows, width), jnp.bfloat16),
        compiler_params=pltpu.CompilerParams(vmem_limit_bytes=16 * 1024 * 1024),
        cost_estimate=pl.CostEstimate(
            flops=3 * rows * width, bytes_accessed=10 * rows * width, transcendentals=0
        ),
    )(*terms)


def permuted(block_input, prenorm_gain, weight, query, grad_normed, qk_gain):
    chips = lax.axis_size("dp") // CORES
    chip = lax.axis_index("dp") // CORES
    core = lax.axis_index("dp") % CORES
    columns = weight.shape[1]
    pair_columns = columns * CORES

    steps = []
    rightward, leftward = weight, weight
    for step in range(1, chips):
        rightward = line_move(rightward, 1, lambda at: at - step + 1 >= 0)
        leftward = line_move(leftward, -1, lambda at: at + step - 1 < chips)
        steps.append((rightward, leftward))

    input_wide_float = block_input.astype(jnp.float32)
    local_sum = jnp.sum(input_wide_float, axis=1)
    local_square = jnp.sum(input_wide_float * input_wide_float, axis=1)
    total_sum, total_square = lax.psum((local_sum, local_square), "mp")
    row_average = (total_sum / D)[:, None]
    reciprocal_deviation = lax.rsqrt((total_square / D)[:, None] - row_average * row_average + EPS)
    standardized_input = (input_wide_float - row_average) * reciprocal_deviation
    prenormed_rows = (standardized_input * prenorm_gain).astype(jnp.bfloat16)
    grad_query, qk_partial = qk_backward(query, grad_normed, qk_gain)

    def chip_columns(offset):
        first = lax.rem(chip + offset + chips, chips) * pair_columns
        return lax.dynamic_slice_in_dim(grad_query, first, pair_columns, 1)

    order = []
    for step in range(1, chips):
        for offset in ((chips - step) % chips, step):
            if offset not in order:
                order.append(offset)
    order.append(0)
    own, theirs = {}, {}
    for offset in order:
        part = lax.dot_general(
            prenormed_rows,
            chip_columns(offset),
            (((0,), (0,)), ((), ())),
            preferred_element_type=jnp.float32,
        )
        own[offset] = lax.dynamic_slice_in_dim(part, core * columns, columns, 1)
        theirs[offset] = partner_swap(
            lax.dynamic_slice_in_dim(part, (1 - core) * columns, columns, 1).astype(jnp.bfloat16)
        )

    to_right, to_left = None, None
    for step in range(1, chips):
        right_terms = [own[chips - step], theirs[chips - step]]
        left_terms = [own[step], theirs[step]]
        if step > 1:
            right_terms.append(to_right)
            left_terms.append(to_left)
        to_right = line_move(add_terms(*right_terms), 1, lambda at: at < step)
        to_left = line_move(add_terms(*left_terms), -1, lambda at: at >= chips - step)
    grad_weight = own[0] + theirs[0].astype(jnp.float32)
    if chips > 1:
        grad_weight = grad_weight + to_right.astype(jnp.float32) + to_left.astype(jnp.float32)

    def product(block, offset):
        other = partner_swap(block)
        first = jnp.where(core == 0, block, other)
        second = jnp.where(core == 0, other, block)
        return lax.dot_general(
            chip_columns(offset),
            jnp.concatenate([first, second], axis=1),
            (((1,), (1,)), ((), ())),
            preferred_element_type=jnp.float32,
        )

    gradient_prenormed_input = product(weight, 0)
    for step in range(1, chips):
        rightward, leftward = steps[step - 1]
        if 2 * step >= chips:
            from_left = chip >= step
            gradient_prenormed_input += product(
                jnp.where(from_left, rightward, leftward), jnp.where(from_left, -step, step)
            )
        else:
            gradient_prenormed_input += product(rightward, -step)
            gradient_prenormed_input += product(leftward, step)

    standardized_gradient = gradient_prenormed_input * prenorm_gain
    slope_mean, slope_cross = lax.psum(
        (
            jnp.sum(standardized_gradient, axis=1),
            jnp.sum(standardized_gradient * standardized_input, axis=1),
        ),
        "mp",
    )
    average_standardized_gradient = (slope_mean / D)[:, None]
    average_cross_term = (slope_cross / D)[:, None]
    input_gradient = (
        reciprocal_deviation
        * (
            standardized_gradient
            - average_standardized_gradient
            - standardized_input * average_cross_term
        )
    ).astype(jnp.bfloat16)
    prenorm_gain_partial = jnp.sum(gradient_prenormed_input * standardized_input, axis=0)
    prenorm_gain_gradient, grad_qk_gain = lax.psum((prenorm_gain_partial, qk_partial), "dp")
    return (input_gradient, grad_weight, prenorm_gain_gradient, grad_qk_gain)


LANES = 128
MESH = pl.DeviceIdType.MESH


def loop(count, body):
    def step(i, carry):
        body(i)
        return carry

    lax.fori_loop(0, count, step, 0)


def aligned(at, size):
    return pl.ds(pl.multiple_of(at * size, size), size)


def fused_kernel(
    sizes,
    x_ref,
    gain_ref,
    w_ref,
    query_ref,
    grad_ref,
    qk_gain_ref,
    input_grad,
    own_grad,
    gain_out,
    qk_out,
    x,
    w,
    query,
    grad,
    gain,
    qk_scale,
    slots,
    grad_query,
    grad_query_out,
    normed_t,
    product,
    product_in,
    average,
    deviation,
    slopes,
    row_sums,
    row_sums_in,
    gain_parts,
    gain_in,
    gain_chips,
    gain_totals,
    qk_part,
    load_sem,
    send_sem,
    recv_sem,
    query_sem,
    normed_sem,
    product_sem,
    sums_sem,
    gain_sem,
):
    dp_count, mp_count, pieces = sizes
    chips = dp_count // CORES
    tokens, rows = x_ref.shape
    columns = w_ref.shape[1]
    piece_rows = rows // pieces
    width = rows * mp_count
    blocks, _, block = product.shape
    row_blocks = tokens // LANES
    heads = columns // LANES

    dp = lax.axis_index("dp")
    mp = lax.axis_index("mp")
    chip = dp // CORES
    core = dp % CORES
    partner = (chip * CORES + 1 - core, mp)

    stages = mp_count.bit_length() - 1

    def mp_peer(stage):
        bit = 1 << stage
        return (dp, mp + bit - 2 * bit * (mp // bit % 2))

    loads = [
        pltpu.make_async_copy(source, target, load_sem.at[i])
        for i, (source, target) in enumerate(
            ((w_ref, w), (x_ref, x), (query_ref, query), (grad_ref, grad), (gain_ref, gain), (qk_gain_ref, qk_scale))
        )
    ]
    for load in loads:
        load.start()

    barrier = pltpu.get_barrier_semaphore()

    def greet(peer):
        pl.semaphore_signal(barrier, inc=1, device_id=peer, device_id_type=MESH)

    def place(way):
        behind = jnp.where(way == 0, chip, chips - 1 - chip)
        return behind, behind < chips - 1

    def next_chip(way):
        return (dp + CORES * (1 - 2 * way), mp)

    def greet_next(way):
        @pl.when(place(way)[1])
        def _():
            greet(next_chip(way))

    loop(2, greet_next)
    greet(partner)
    for stage in range(stages):
        greet(mp_peer(stage))
    loads[0].wait()
    ends = jnp.where(chip == 0, 1, 0) + jnp.where(chip == chips - 1, 1, 0)
    pl.semaphore_wait(barrier, stages + 3 - ends)

    def hop(way, slot, piece, source):
        part = aligned(piece, piece_rows)
        return pltpu.make_async_remote_copy(
            src_ref=source.at[part],
            dst_ref=slots.at[way, slot, part],
            send_sem=send_sem.at[way, slot, piece],
            recv_sem=recv_sem.at[way, slot, piece],
            device_id=next_chip(way),
            device_id_type=MESH,
        )

    def arrival(way, slot, piece):
        return hop(way, slot, piece, slots.at[way, slot])

    def send_weight(piece):
        def one(way):
            @pl.when(place(way)[1])
            def _():
                hop(way, 0, piece, w).start()

        loop(2, one)

    loop(pieces, send_weight)

    def exchange(kind, stage):
        return pltpu.make_async_remote_copy(
            src_ref=row_sums.at[kind, stage],
            dst_ref=row_sums_in.at[kind, stage],
            send_sem=sums_sem.at[kind, 0, stage],
            recv_sem=sums_sem.at[kind, 1, stage],
            device_id=mp_peer(stage),
            device_id_type=MESH,
        )

    def add_stage(kind, stage):
        exchange(kind, stage).wait()
        total = row_sums[kind, stage] + row_sums_in[kind, stage]
        if stage + 1 == stages:
            return total * (1.0 / width)
        row_sums[kind, stage + 1] = total
        exchange(kind, stage + 1).start()

    diagonal = lax.broadcasted_iota(jnp.int32, (LANES, LANES), 0) == lax.broadcasted_iota(
        jnp.int32, (LANES, LANES), 1
    )

    def as_row(tile):
        total = jnp.sum(tile, axis=1, keepdims=True)
        return jnp.sum(jnp.where(diagonal, total, 0.0), axis=0, keepdims=True)

    def as_tile(row):
        total = jnp.sum(jnp.where(diagonal, row, 0.0), axis=1, keepdims=True)
        return jnp.broadcast_to(total, (LANES, LANES))

    loads[1].wait()

    def input_sums(at):
        part = aligned(at, LANES)
        total = jnp.zeros((LANES, LANES), jnp.float32)
        square = jnp.zeros((LANES, LANES), jnp.float32)
        for k in range(rows // LANES):
            value = x[part, k * LANES : (k + 1) * LANES].astype(jnp.float32)
            total += value
            square += value * value
        row_sums[0, 0, pl.ds(at, 1), :] = as_row(total)
        row_sums[0, 0, pl.ds(row_blocks + at, 1), :] = as_row(square)

    loop(row_blocks, input_sums)
    exchange(0, 0).start()

    for load in loads[2:]:
        load.wait()
    qk_gain = qk_scale[...].reshape(1, LANES)
    qk_part[...] = jnp.zeros_like(qk_part)
    chunk = 64

    def qk_columns(to_chip, half, target):
        first = (to_chip * CORES + half) * columns

        def some_rows(at):
            part = aligned(at, chunk)
            total = jnp.zeros_like(qk_part)
            for head in range(heads):
                lanes = pl.ds(pl.multiple_of(first + head * LANES, LANES), LANES)
                q_float = query[part, lanes].astype(jnp.float32)
                upstream = grad[part, lanes].astype(jnp.float32)
                q_mean = jnp.mean(q_float, axis=1, keepdims=True)
                q_var = jnp.mean(q_float * q_float, axis=1, keepdims=True) - q_mean * q_mean
                q_inv = lax.rsqrt(q_var + EPS)
                qhat = (q_float - q_mean) * q_inv
                dqhat = upstream * qk_gain
                dq_mean = jnp.mean(dqhat, axis=1, keepdims=True)
                dq_cross = jnp.mean(dqhat * qhat, axis=1, keepdims=True)
                out = q_inv * (dqhat - dq_mean - qhat * dq_cross)
                target[to_chip, part, head * LANES : (head + 1) * LANES] = out.astype(jnp.bfloat16)
                total += jnp.sum((upstream * qhat).reshape(-1, 8, LANES), axis=0)
            qk_part[...] += total

        loop(tokens // chunk, some_rows)

    def share_query(to_chip):
        return pltpu.make_async_remote_copy(
            src_ref=grad_query_out.at[to_chip],
            dst_ref=grad_query.at[to_chip, pl.ds(tokens, tokens)],
            send_sem=query_sem.at[0, to_chip],
            recv_sem=query_sem.at[1, to_chip],
            device_id=partner,
            device_id_type=MESH,
        )

    def partner_columns(to_chip):
        qk_columns(to_chip, 1 - core, grad_query_out)
        share_query(to_chip).start()

    loop(chips, partner_columns)
    for stage in range(stages - 1):
        add_stage(0, stage)
    loop(chips, lambda to_chip: qk_columns(to_chip, core, grad_query))

    sums = add_stage(0, stages - 1)
    means = sums[:row_blocks]
    scales = lax.rsqrt(sums[row_blocks:] - means * means + EPS)
    for at in range(row_blocks):
        average[at * LANES : (at + 1) * LANES, :] = as_tile(means[at : at + 1])
        deviation[at * LANES : (at + 1) * LANES, :] = as_tile(scales[at : at + 1])

    def standardized(part, lanes):
        return (x[part, lanes].astype(jnp.float32) - average[part, :]) * deviation[part, :]

    def share_normed(piece):
        part = aligned(piece, piece_rows)
        return pltpu.make_async_remote_copy(
            src_ref=normed_t.at[0, part],
            dst_ref=normed_t.at[1, part],
            send_sem=normed_sem.at[0, piece],
            recv_sem=normed_sem.at[1, piece],
            device_id=partner,
            device_id_type=MESH,
        )

    def normalize(piece):
        def some_lanes(k):
            lanes = aligned(piece * (piece_rows // LANES) + k, LANES)
            scale = gain[lanes].reshape(1, LANES)
            for at in range(row_blocks):
                part = slice(at * LANES, (at + 1) * LANES)
                value = standardized(part, lanes) * scale
                normed_t[0, lanes, part] = value.T.astype(jnp.bfloat16)

        loop(piece_rows // LANES, some_lanes)
        share_normed(piece).start()

    loop(pieces, normalize)

    loop(chips, lambda to_chip: share_query(to_chip).wait_recv())
    loop(pieces, lambda piece: share_normed(piece).wait_recv())

    def contribution(part, to_chip):
        def half(which):
            return jnp.dot(
                normed_t[which, part, :],
                grad_query[to_chip, which * tokens : (which + 1) * tokens, :],
                preferred_element_type=jnp.float32,
            )

        return half(0) + half(1)

    def weight_product(from_chip, weight, first):
        def some_rows(at):
            value = lax.dot_general(
                grad_query[from_chip],
                weight[aligned(at, block), :],
                (((1,), (1,)), ((), ())),
                preferred_element_type=jnp.float32,
            )
            if first:
                product[at] = value
            else:
                product[at] += value

        loop(blocks, some_rows)

    def give(slot, piece):
        def one(way):
            @pl.when(place(way)[1])
            def _():
                hop(way, slot + 1, piece, slots.at[way, slot]).start()

        loop(2, one)

    def slot_step(slot):
        def piece_step(piece):
            part = aligned(piece, piece_rows)

            def take(way):
                behind, ahead = place(way)

                @pl.when(behind > 0)
                def _():
                    arrival(way, slot, piece).wait_recv()

                @pl.when(ahead & (slot >= behind))
                def _():
                    skip = slot - behind
                    to_chip = jnp.where(way == 0, chips - 1 - skip, skip)
                    own = contribution(part, to_chip)

                    @pl.when(behind > 0)
                    def _():
                        held = slots[way, slot, part, :].astype(jnp.float32)
                        slots[way, slot, part, :] = (held + own).astype(jnp.bfloat16)

                    @pl.when(behind == 0)
                    def _():
                        slots[way, slot, part, :] = own.astype(jnp.bfloat16)

            loop(2, take)

            @pl.when((slot < chips - 2) | (piece < pieces - 1))
            def _():
                give(slot, piece)

        loop(pieces, piece_step)

        @pl.when(slot == 0)
        def _():
            weight_product(chip, w, True)

            def own_piece(piece):
                part = aligned(piece, piece_rows)
                own_grad[part, :] = contribution(part, chip)

            loop(pieces, own_piece)

        def use_weight(way):
            behind, _ = place(way)

            @pl.when(slot < behind)
            def _():
                from_chip = jnp.where(way == 0, chip - 1 - slot, chip + 1 + slot)
                weight_product(from_chip, slots.at[way, slot], False)

        loop(2, use_weight)

    loop(chips - 1, slot_step)

    def share_product(at):
        return pltpu.make_async_remote_copy(
            src_ref=product.at[at, pl.ds(tokens, tokens)],
            dst_ref=product_in.at[at],
            send_sem=product_sem.at[0, at],
            recv_sem=product_sem.at[1, at],
            device_id=partner,
            device_id_type=MESH,
        )

    loop(blocks, lambda at: share_product(at).start())

    gain_rows = rows // LANES
    half_rows = gain_parts.shape[1]
    slopes[...] = jnp.zeros_like(slopes)
    per_block = block // LANES

    def slope_sums(at):
        share_product(at).wait_recv()
        for k in range(per_block):
            inner = slice(k * LANES, (k + 1) * LANES)
            lanes = aligned(at * per_block + k, LANES)
            scale = gain[lanes].reshape(1, LANES)

            def some_rows(row, gain_total):
                part = aligned(row, LANES)
                value = product[at, part, inner] + product_in[at, part, inner]
                product[at, part, inner] = value
                xhat = standardized(part, lanes)
                slope = value * scale
                slopes[0, part, :] += slope
                slopes[1, part, :] += slope * xhat
                return gain_total + jnp.sum((value * xhat).reshape(-1, 8, LANES), axis=0)

            gain_total = lax.fori_loop(0, row_blocks, some_rows, jnp.zeros((8, LANES), jnp.float32))
            gain_parts[(at * per_block + k) // half_rows, pl.ds((at * per_block + k) % half_rows, 1), :] = jnp.sum(gain_total, axis=0, keepdims=True)

    loop(blocks, slope_sums)
    for at in range(gain_rows, CORES * half_rows):
        total = jnp.sum(qk_part[...], axis=0, keepdims=True)
        row = total if at == gain_rows else jnp.zeros_like(total)
        gain_parts[at // half_rows, at % half_rows : at % half_rows + 1, :] = row

    def swap_gains(source, target, index):
        return pltpu.make_async_remote_copy(
            src_ref=source,
            dst_ref=target,
            send_sem=gain_sem.at[0, index],
            recv_sem=gain_sem.at[1, index],
            device_id=partner,
            device_id_type=MESH,
        )

    def spread_gains(k):
        mine = gain_chips.at[chip]
        return pltpu.make_async_remote_copy(
            src_ref=mine,
            dst_ref=mine,
            send_sem=gain_sem.at[0, k],
            recv_sem=gain_sem.at[1, k],
            device_id=(lax.rem(dp + CORES * k, dp_count), mp),
            device_id_type=MESH,
        )

    first_swap = swap_gains(gain_parts.at[1 - core], gain_in, 0)
    first_swap.start()
    for at in range(row_blocks):
        part = slice(at * LANES, (at + 1) * LANES)
        row_sums[1, 0, at : at + 1, :] = as_row(slopes[0, part, :])
        row_sums[1, 0, row_blocks + at : row_blocks + at + 1, :] = as_row(slopes[1, part, :])
    exchange(1, 0).start()
    first_swap.wait()
    gain_chips[chip] = gain_parts[core] + gain_in[...]
    loop(chips - 1, lambda k: spread_gains(k + 1).start())
    give(chips - 2, pieces - 1)
    for stage in range(stages - 1):
        add_stage(1, stage)
    sums = add_stage(1, stages - 1)
    for at in range(row_blocks):
        part = slice(at * LANES, (at + 1) * LANES)
        slopes[0, part, :] = as_tile(sums[at : at + 1])
        slopes[1, part, :] = as_tile(sums[row_blocks + at : row_blocks + at + 1])

    def finish_rows(row):
        part = aligned(row, LANES)
        for k in range(gain_rows):
            lanes = slice(k * LANES, (k + 1) * LANES)
            at, inner = k // per_block, k % per_block * LANES
            slope = product[at, part, inner : inner + LANES] * gain[lanes].reshape(1, LANES)
            value = deviation[part, :] * (
                slope - slopes[0, part, :] - standardized(part, lanes) * slopes[1, part, :]
            )
            input_grad[part, lanes] = value.astype(jnp.bfloat16)

    loop(row_blocks, finish_rows)

    loop(chips - 1, lambda k: spread_gains(k + 1).wait())
    gain_totals[core] = lax.fori_loop(1, chips, lambda k, total: total + gain_chips[k], gain_chips[0])
    total = gain_totals.at[core]
    last_swap = swap_gains(total, total, chips)
    last_swap.start()
    last_swap.wait()
    for k in range(gain_rows):
        gain_out[k * LANES : (k + 1) * LANES] = gain_totals[k // half_rows, k % half_rows]
    qk_out[...] = gain_totals[gain_rows // half_rows, gain_rows % half_rows]

    def finish_piece(piece):
        part = aligned(piece, piece_rows)

        def one(way):
            @pl.when(place(way)[0] > 0)
            def _():
                arrival(way, chips - 1, piece).wait_recv()
                own_grad[part, :] += slots[way, chips - 1, part, :].astype(jnp.float32)

        loop(2, one)

    loop(pieces, finish_piece)

    loop(chips, lambda to_chip: share_query(to_chip).wait_send())
    loop(pieces, lambda piece: share_normed(piece).wait_send())
    loop(blocks, lambda at: share_product(at).wait_send())

    def sent(way):
        @pl.when(place(way)[1])
        def _():
            def of_slot(slot):
                loop(pieces, lambda piece: arrival(way, slot, piece).wait_send())

            loop(chips, of_slot)

    loop(2, sent)


def write_kernel(parts, *refs):
    count = len(refs) // 2
    sources, targets, sem = refs[:count], refs[count:-1], refs[-1]
    copies = []
    for source, target in zip(sources, targets):
        pieces = parts if len(source.shape) > 1 else 1
        size = source.shape[0] // pieces
        for i in range(pieces):
            part = pl.ds(i * size, size)
            copies.append(pltpu.make_async_copy(source.at[part], target.at[part], sem.at[len(copies)]))
    for copy in copies:
        copy.start()
    for copy in copies:
        copy.wait()


def fused(block_input, prenorm_gain, weight, query, grad_normed, qk_gain):
    dp_count, mp_count = lax.axis_size("dp"), lax.axis_size("mp")
    chips = dp_count // CORES
    tokens, rows = block_input.shape
    columns = weight.shape[1]
    features = query.shape[1]
    pieces = next(count for count in (3, 2, 1) if rows // LANES % count == 0)
    block = math.gcd(rows, 2 * LANES)
    gain_rows = -(-(rows // LANES + 1) // (8 * CORES)) * 8
    stages = mp_count.bit_length() - 1
    anywhere = pl.BlockSpec(memory_space=pl.ANY)
    local = pl.BlockSpec(memory_space=pltpu.VMEM)
    bf16, f32 = jnp.bfloat16, jnp.float32
    dma = pltpu.SemaphoreType.DMA
    results = pl.pallas_call(
        functools.partial(fused_kernel, (dp_count, mp_count, pieces)),
        in_specs=[anywhere] * 6,
        out_specs=[local] * 4,
        out_shape=[
            pltpu.VMEM((tokens, rows), bf16),
            pltpu.VMEM((rows, columns), f32),
            pltpu.VMEM((rows,), f32),
            pltpu.VMEM((LANES,), f32),
        ],
        scratch_shapes=[
            pltpu.VMEM((tokens, rows), bf16),
            pltpu.VMEM((rows, columns), bf16),
            pltpu.VMEM((tokens, features), bf16),
            pltpu.VMEM((tokens, features), bf16),
            pltpu.VMEM((rows,), f32),
            pltpu.VMEM((LANES,), f32),
            pltpu.VMEM((2, chips, rows, columns), bf16),
            pltpu.VMEM((chips, CORES * tokens, columns), bf16),
            pltpu.VMEM((chips, tokens, columns), bf16),
            pltpu.VMEM((CORES, rows, tokens), bf16),
            pltpu.VMEM((rows // block, CORES * tokens, block), f32),
            pltpu.VMEM((rows // block, tokens, block), f32),
            pltpu.VMEM((tokens, LANES), f32),
            pltpu.VMEM((tokens, LANES), f32),
            pltpu.VMEM((2, tokens, LANES), f32),
            pltpu.VMEM((2, stages, 2 * tokens // LANES, LANES), f32),
            pltpu.VMEM((2, stages, 2 * tokens // LANES, LANES), f32),
            pltpu.VMEM((CORES, gain_rows, LANES), f32),
            pltpu.VMEM((gain_rows, LANES), f32),
            pltpu.VMEM((chips, gain_rows, LANES), f32),
            pltpu.VMEM((CORES, gain_rows, LANES), f32),
            pltpu.VMEM((8, LANES), f32),
            dma((6,)),
            dma((2, chips, pieces)),
            dma((2, chips, pieces)),
            dma((2, chips)),
            dma((2, pieces)),
            dma((2, rows // block)),
            dma((2, 2, stages)),
            dma((2, chips + 1)),
        ],
        compiler_params=pltpu.CompilerParams(
            collective_id=0, has_side_effects=True, vmem_limit_bytes=56 * 1024 * 1024
        ),
        cost_estimate=pl.CostEstimate(
            flops=8 * tokens * rows * features, bytes_accessed=8 * tokens * features, transcendentals=0
        ),
    )(block_input, prenorm_gain, weight, query, grad_normed, qk_gain)
    parts = 4
    return pl.pallas_call(
        functools.partial(write_kernel, parts),
        in_specs=[local] * 4,
        out_specs=[anywhere] * 4,
        out_shape=[jax.ShapeDtypeStruct(result.shape, result.dtype) for result in results],
        scratch_shapes=[dma((2 * parts + 2,))],
        compiler_params=pltpu.CompilerParams(vmem_limit_bytes=4 * 1024 * 1024),
    )(*[pltpu.with_memory_space_constraint(result, pltpu.VMEM) for result in results])


def shards(block_input, prenorm_gain, weight, query, grad_normed, qk_gain):
    tokens, rows = block_input.shape
    sizes = (tokens, rows, weight.shape[1])
    whole_tiles = all(size % LANES == 0 for size in sizes) and qk_gain.shape[0] == LANES
    mp_count = lax.axis_size("mp")
    several = lax.axis_size("dp") > CORES and mp_count > 1 and mp_count & (mp_count - 1) == 0
    body = fused if whole_tiles and several else permuted
    return body(block_input, prenorm_gain, weight, query, grad_normed, qk_gain)


def solution(mesh):
    return jax.shard_map(
        shards,
        mesh=mesh,
        in_specs=(P("dp", "mp"), P("mp"), P("mp", "dp"), P("dp", None), P("dp", None), P()),
        out_specs=(P("dp", "mp"), P("mp", "dp"), P("mp"), P()),
        check_vma=False,
    )
```

```python
import functools
import math

import jax
import jax.numpy as jnp
from jax import lax
from jax.experimental import pallas as pl
from jax.experimental.pallas import tpu as pltpu
from jax.sharding import PartitionSpec as P

D = 6144


EPS = 1e-06


def qk_kernel(query_ref, grad_ref, gain_ref, out_ref, contrib_ref):
    @pl.when(pl.program_id(0) == 0)
    def _():
        contrib_ref[...] = jnp.zeros_like(contrib_ref)

    head_size = gain_ref.shape[1]
    gain = gain_ref[...]
    total = jnp.zeros_like(contrib_ref)
    for head in range(query_ref.shape[1] // head_size):
        columns = pl.ds(head * head_size, head_size)
        q_float = query_ref[:, columns].astype(jnp.float32)
        upstream = grad_ref[:, columns].astype(jnp.float32)
        q_mean = jnp.mean(q_float, axis=1, keepdims=True)
        q_var = jnp.mean(q_float * q_float, axis=1, keepdims=True) - q_mean * q_mean
        q_inv = lax.rsqrt(q_var + EPS)
        qhat = (q_float - q_mean) * q_inv
        dqhat = upstream * gain
        dq_mean = jnp.mean(dqhat, axis=1, keepdims=True)
        dq_cross = jnp.mean(dqhat * qhat, axis=1, keepdims=True)
        out_ref[:, columns] = (q_inv * (dqhat - dq_mean - qhat * dq_cross)).astype(out_ref.dtype)
        product = upstream * qhat
        total += jnp.sum(product.reshape(-1, 8, head_size), axis=0)
    contrib_ref[...] += total


def qk_backward(query, grad_normed, qk_gain):
    rows, width = query.shape
    head_size = qk_gain.shape[0]
    block = min(rows, 64)
    grad_query, contrib = pl.pallas_call(
        qk_kernel,
        grid=(rows // block,),
        in_specs=[
            pl.BlockSpec((block, width), lambda i: (i, 0)),
            pl.BlockSpec((block, width), lambda i: (i, 0)),
            pl.BlockSpec((1, head_size), lambda i: (0, 0)),
        ],
        out_specs=[
            pl.BlockSpec((block, width), lambda i: (i, 0)),
            pl.BlockSpec((8, head_size), lambda i: (0, 0)),
        ],
        out_shape=[
            jax.ShapeDtypeStruct((rows, width), jnp.bfloat16),
            jax.ShapeDtypeStruct((8, head_size), jnp.float32),
        ],
        compiler_params=pltpu.CompilerParams(vmem_limit_bytes=32 * 1024 * 1024),
        cost_estimate=pl.CostEstimate(flops=40 * rows * width, bytes_accessed=6 * rows * width, transcendentals=0),
    )(query, grad_normed, qk_gain.reshape(1, -1))
    return grad_query, jnp.sum(contrib, axis=0)


CORES = 2


def line_move(value, shift, valid):
    chips = lax.axis_size("dp") // CORES
    pairs = [
        (chip * CORES + core, (chip + shift) * CORES + core)
        for chip in range(chips)
        for core in range(CORES)
        if 0 <= chip + shift < chips and valid(chip)
    ]
    return lax.ppermute(value, "dp", pairs)


def partner_swap(value):
    count = lax.axis_size("dp")
    pairs = [(at, at - at % CORES + (at + 1) % CORES) for at in range(count)]
    return lax.ppermute(value, "dp", pairs)


def add_kernel(*refs):
    total = refs[0][...]
    for ref in refs[1:-1]:
        total = total + ref[...].astype(jnp.float32)
    refs[-1][...] = total.astype(jnp.bfloat16)


def add_terms(*terms):
    rows, width = terms[0].shape
    block = math.gcd(rows, 256)
    spec = pl.BlockSpec((block, width), lambda i: (i, 0))
    return pl.pallas_call(
        add_kernel,
        grid=(rows // block,),
        in_specs=[spec] * len(terms),
        out_specs=spec,
        out_shape=jax.ShapeDtypeStruct((rows, width), jnp.bfloat16),
        compiler_params=pltpu.CompilerParams(vmem_limit_bytes=16 * 1024 * 1024),
        cost_estimate=pl.CostEstimate(
            flops=3 * rows * width, bytes_accessed=10 * rows * width, transcendentals=0
        ),
    )(*terms)


def permuted(block_input, prenorm_gain, weight, query, grad_normed, qk_gain):
    chips = lax.axis_size("dp") // CORES
    chip = lax.axis_index("dp") // CORES
    core = lax.axis_index("dp") % CORES
    columns = weight.shape[1]
    pair_columns = columns * CORES

    steps = []
    rightward, leftward = weight, weight
    for step in range(1, chips):
        rightward = line_move(rightward, 1, lambda at: at - step + 1 >= 0)
        leftward = line_move(leftward, -1, lambda at: at + step - 1 < chips)
        steps.append((rightward, leftward))

    input_wide_float = block_input.astype(jnp.float32)
    local_sum = jnp.sum(input_wide_float, axis=1)
    local_square = jnp.sum(input_wide_float * input_wide_float, axis=1)
    total_sum, total_square = lax.psum((local_sum, local_square), "mp")
    row_average = (total_sum / D)[:, None]
    reciprocal_deviation = lax.rsqrt((total_square / D)[:, None] - row_average * row_average + EPS)
    standardized_input = (input_wide_float - row_average) * reciprocal_deviation
    prenormed_rows = (standardized_input * prenorm_gain).astype(jnp.bfloat16)
    grad_query, qk_partial = qk_backward(query, grad_normed, qk_gain)

    def chip_columns(offset):
        first = lax.rem(chip + offset + chips, chips) * pair_columns
        return lax.dynamic_slice_in_dim(grad_query, first, pair_columns, 1)

    order = []
    for step in range(1, chips):
        for offset in ((chips - step) % chips, step):
            if offset not in order:
                order.append(offset)
    order.append(0)
    own, theirs = {}, {}
    for offset in order:
        part = lax.dot_general(
            prenormed_rows,
            chip_columns(offset),
            (((0,), (0,)), ((), ())),
            preferred_element_type=jnp.float32,
        )
        own[offset] = lax.dynamic_slice_in_dim(part, core * columns, columns, 1)
        theirs[offset] = partner_swap(
            lax.dynamic_slice_in_dim(part, (1 - core) * columns, columns, 1).astype(jnp.bfloat16)
        )

    to_right, to_left = None, None
    for step in range(1, chips):
        right_terms = [own[chips - step], theirs[chips - step]]
        left_terms = [own[step], theirs[step]]
        if step > 1:
            right_terms.append(to_right)
            left_terms.append(to_left)
        to_right = line_move(add_terms(*right_terms), 1, lambda at: at < step)
        to_left = line_move(add_terms(*left_terms), -1, lambda at: at >= chips - step)
    grad_weight = own[0] + theirs[0].astype(jnp.float32)
    if chips > 1:
        grad_weight = grad_weight + to_right.astype(jnp.float32) + to_left.astype(jnp.float32)

    def product(block, offset):
        other = partner_swap(block)
        first = jnp.where(core == 0, block, other)
        second = jnp.where(core == 0, other, block)
        return lax.dot_general(
            chip_columns(offset),
            jnp.concatenate([first, second], axis=1),
            (((1,), (1,)), ((), ())),
            preferred_element_type=jnp.float32,
        )

    gradient_prenormed_input = product(weight, 0)
    for step in range(1, chips):
        rightward, leftward = steps[step - 1]
        if 2 * step >= chips:
            from_left = chip >= step
            gradient_prenormed_input += product(
                jnp.where(from_left, rightward, leftward), jnp.where(from_left, -step, step)
            )
        else:
            gradient_prenormed_input += product(rightward, -step)
            gradient_prenormed_input += product(leftward, step)

    standardized_gradient = gradient_prenormed_input * prenorm_gain
    slope_mean, slope_cross = lax.psum(
        (
            jnp.sum(standardized_gradient, axis=1),
            jnp.sum(standardized_gradient * standardized_input, axis=1),
        ),
        "mp",
    )
    average_standardized_gradient = (slope_mean / D)[:, None]
    average_cross_term = (slope_cross / D)[:, None]
    input_gradient = (
        reciprocal_deviation
        * (
            standardized_gradient
            - average_standardized_gradient
            - standardized_input * average_cross_term
        )
    ).astype(jnp.bfloat16)
    prenorm_gain_partial = jnp.sum(gradient_prenormed_input * standardized_input, axis=0)
    prenorm_gain_gradient, grad_qk_gain = lax.psum((prenorm_gain_partial, qk_partial), "dp")
    return (input_gradient, grad_weight, prenorm_gain_gradient, grad_qk_gain)


LANES = 128
MESH = pl.DeviceIdType.MESH


def loop(count, body):
    def step(i, carry):
        body(i)
        return carry

    lax.fori_loop(0, count, step, 0)


def aligned(at, size):
    return pl.ds(pl.multiple_of(at * size, size), size)


def fused_kernel(
    sizes,
    x_ref,
    gain_ref,
    w_ref,
    query_ref,
    grad_ref,
    qk_gain_ref,
    input_grad,
    own_grad,
    gain_out,
    qk_out,
    x,
    w,
    queries,
    gain,
    qk_scale,
    slots,
    grad_query,
    grad_query_out,
    normed_t,
    product,
    product_in,
    average,
    deviation,
    slopes,
    row_sums,
    row_sums_in,
    gain_parts,
    gain_in,
    gain_chips,
    gain_totals,
    qk_part,
    load_sem,
    weight_sem,
    ready_sem,
    send_sem,
    recv_sem,
    query_sem,
    normed_sem,
    product_sem,
    sums_sem,
    gain_sem,
):
    dp_count, mp_count, pieces = sizes
    chips = dp_count // CORES
    tokens, rows = x_ref.shape
    columns = w_ref.shape[1]
    piece_rows = rows // pieces
    width = rows * mp_count
    blocks, _, block = product.shape
    row_blocks = tokens // LANES
    heads = columns // LANES

    dp = lax.axis_index("dp")
    mp = lax.axis_index("mp")
    chip = dp // CORES
    core = dp % CORES
    partner = (chip * CORES + 1 - core, mp)

    stages = mp_count.bit_length() - 1

    def mp_peer(stage):
        bit = 1 << stage
        return (dp, mp + bit - 2 * bit * (mp // bit % 2))

    def load_weight(piece):
        part = aligned(piece, piece_rows)
        return pltpu.make_async_copy(w_ref.at[part], w.at[part], weight_sem.at[piece])

    loop(pieces, lambda piece: load_weight(piece).start())

    barrier = pltpu.get_barrier_semaphore()

    def place(way):
        behind = jnp.where(way == 0, chip, chips - 1 - chip)
        return behind, behind < chips - 1

    def next_chip(way):
        return (dp + CORES * (1 - 2 * way), mp)

    def tell(semaphore, peer):
        pl.semaphore_signal(semaphore, inc=1, device_id=peer, device_id_type=MESH)

    pairs = [(chip > 0, next_chip(1), chip < chips - 1, next_chip(0)), (core == 1, partner, core == 0, partner)]
    for stage in range(stages):
        low = mp // (1 << stage) % 2 == 0
        pairs.append((~low, mp_peer(stage), low, mp_peer(stage)))
    for _, _, below, peer in pairs:
        @pl.when(below)
        def _():
            tell(barrier, peer)

    above_count = sum(jnp.where(above, 1, 0) for above, _, _, _ in pairs)

    @pl.when(above_count > 0)
    def _():
        pl.semaphore_wait(barrier, above_count)

    for k, (above, peer, _, _) in enumerate(pairs):
        @pl.when(above)
        def _():
            tell(ready_sem.at[k], peer)

    def await_ready(k):
        @pl.when(pairs[k][2])
        def _():
            pl.semaphore_wait(ready_sem.at[k], 1)

    def hop(way, slot, piece, source):
        part = aligned(piece, piece_rows)
        return pltpu.make_async_remote_copy(
            src_ref=source.at[part],
            dst_ref=slots.at[way, slot, part],
            send_sem=send_sem.at[way],
            recv_sem=recv_sem.at[way, slot, piece],
            device_id=next_chip(way),
            device_id_type=MESH,
        )

    def arrival(way, slot, piece):
        return hop(way, slot, piece, slots.at[way, slot])

    def send_weight(piece, way):
        @pl.when(place(way)[1])
        def _():
            hop(way, 0, piece, w).start()

    def load_and_send(piece):
        load_weight(piece).wait()
        send_weight(piece, 1)

    loop(pieces, load_and_send)
    await_ready(0)
    loop(pieces, lambda piece: send_weight(piece, 0))

    loads = [
        pltpu.make_async_copy(source, target, load_sem.at[i])
        for i, (source, target) in enumerate(
            ((x_ref, x), (gain_ref, gain), (qk_gain_ref, qk_scale))
        )
    ]
    for load in loads:
        load.start()
    for k, source in enumerate((query_ref, grad_ref)):
        pltpu.make_async_copy(source, queries.at[k], load_sem.at[3]).start()

    def exchange(kind, stage):
        return pltpu.make_async_remote_copy(
            src_ref=row_sums.at[kind, stage],
            dst_ref=row_sums_in.at[kind, stage],
            send_sem=sums_sem.at[0],
            recv_sem=sums_sem.at[1 + kind * stages + stage],
            device_id=mp_peer(stage),
            device_id_type=MESH,
        )

    def add_stage(kind, stage):
        exchange(kind, stage).wait()
        total = row_sums[kind, stage] + row_sums_in[kind, stage]
        if stage + 1 == stages:
            return total * (1.0 / width)
        row_sums[kind, stage + 1] = total
        exchange(kind, stage + 1).start()

    diagonal = lax.broadcasted_iota(jnp.int32, (LANES, LANES), 0) == lax.broadcasted_iota(
        jnp.int32, (LANES, LANES), 1
    )

    def as_row(tile):
        total = jnp.sum(tile, axis=1, keepdims=True)
        return jnp.sum(jnp.where(diagonal, total, 0.0), axis=0, keepdims=True)

    def as_tile(row):
        total = jnp.sum(jnp.where(diagonal, row, 0.0), axis=1, keepdims=True)
        return jnp.broadcast_to(total, (LANES, LANES))

    loads[0].wait()

    def input_sums(at):
        part = aligned(at, LANES)
        total = jnp.zeros((LANES, LANES), jnp.float32)
        square = jnp.zeros((LANES, LANES), jnp.float32)
        for k in range(rows // LANES):
            value = x[part, k * LANES : (k + 1) * LANES].astype(jnp.float32)
            total += value
            square += value * value
        row_sums[0, 0, pl.ds(at, 1), :] = as_row(total)
        row_sums[0, 0, pl.ds(row_blocks + at, 1), :] = as_row(square)

    loop(row_blocks, input_sums)
    for k in range(1, len(pairs)):
        await_ready(k)
    exchange(0, 0).start()

    for load in loads[1:]:
        load.wait()
    pltpu.make_async_copy(queries, queries, load_sem.at[3]).wait()
    qk_gain = qk_scale[...].reshape(1, LANES)
    qk_part[...] = jnp.zeros_like(qk_part)
    chunk = 64

    def qk_columns(to_chip, half, target):
        first = (to_chip * CORES + half) * columns

        def some_rows(at):
            part = aligned(at, chunk)
            total = jnp.zeros_like(qk_part)
            for head in range(heads):
                lanes = pl.ds(pl.multiple_of(first + head * LANES, LANES), LANES)
                q_float = queries[0, part, lanes].astype(jnp.float32)
                upstream = queries[1, part, lanes].astype(jnp.float32)
                q_mean = jnp.mean(q_float, axis=1, keepdims=True)
                q_var = jnp.mean(q_float * q_float, axis=1, keepdims=True) - q_mean * q_mean
                q_inv = lax.rsqrt(q_var + EPS)
                qhat = (q_float - q_mean) * q_inv
                dqhat = upstream * qk_gain
                dq_mean = jnp.mean(dqhat, axis=1, keepdims=True)
                dq_cross = jnp.mean(dqhat * qhat, axis=1, keepdims=True)
                out = q_inv * (dqhat - dq_mean - qhat * dq_cross)
                target[to_chip, part, head * LANES : (head + 1) * LANES] = out.astype(jnp.bfloat16)
                total += jnp.sum((upstream * qhat).reshape(-1, 8, LANES), axis=0)
            qk_part[...] += total

        loop(tokens // chunk, some_rows)

    def share(source, target, sem, index=0):
        return pltpu.make_async_remote_copy(
            src_ref=source,
            dst_ref=target,
            send_sem=sem.at[0],
            recv_sem=sem.at[1 + index],
            device_id=partner,
            device_id_type=MESH,
        )

    def share_query(which):
        return share(grad_query_out.at[which], grad_query.at[which, pl.ds(tokens, tokens)], query_sem)

    def partner_columns(to_chip):
        qk_columns(to_chip, 1 - core, grad_query_out)
        share_query(to_chip).start()

    loop(chips, partner_columns)
    for stage in range(stages - 1):
        add_stage(0, stage)
    loop(chips, lambda to_chip: qk_columns(to_chip, core, grad_query))

    sums = add_stage(0, stages - 1)
    means = sums[:row_blocks]
    scales = lax.rsqrt(sums[row_blocks:] - means * means + EPS)
    for at in range(row_blocks):
        average[at * LANES : (at + 1) * LANES, :] = as_tile(means[at : at + 1])
        deviation[at * LANES : (at + 1) * LANES, :] = as_tile(scales[at : at + 1])

    def standardized(part, lanes):
        return (x[part, lanes].astype(jnp.float32) - average[part, :]) * deviation[part, :]

    def share_normed(part):
        return share(normed_t.at[0, part], normed_t.at[1, part], normed_sem)

    def normalize(piece):
        def some_lanes(k):
            lanes = aligned(piece * (piece_rows // LANES) + k, LANES)
            scale = gain[lanes].reshape(1, LANES)
            for at in range(row_blocks):
                part = slice(at * LANES, (at + 1) * LANES)
                value = standardized(part, lanes) * scale
                normed_t[0, lanes, part] = value.T.astype(jnp.bfloat16)

        loop(piece_rows // LANES, some_lanes)
        share_normed(aligned(piece, piece_rows)).start()

    loop(pieces, normalize)

    share_query(slice(None)).wait_recv()
    share_normed(slice(None)).wait_recv()

    def contribution(part, to_chip):
        def half(which):
            return jnp.dot(
                normed_t[which, part, :],
                grad_query[to_chip, which * tokens : (which + 1) * tokens, :],
                preferred_element_type=jnp.float32,
            )

        return half(0) + half(1)

    def weight_product(from_chip, weight, first):
        def some_rows(at):
            value = lax.dot_general(
                grad_query[from_chip],
                weight[aligned(at, block), :],
                (((1,), (1,)), ((), ())),
                preferred_element_type=jnp.float32,
            )
            if first:
                product[at] = value
            else:
                product[at] += value

        loop(blocks, some_rows)

    def give(slot, piece):
        def one(way):
            @pl.when(place(way)[1])
            def _():
                hop(way, slot + 1, piece, slots.at[way, slot]).start()

        loop(2, one)

    def slot_step(slot):
        def piece_step(piece):
            part = aligned(piece, piece_rows)

            def take(way):
                behind, ahead = place(way)

                @pl.when(behind > 0)
                def _():
                    arrival(way, slot, piece).wait_recv()

                @pl.when(ahead & (slot >= behind))
                def _():
                    skip = slot - behind
                    to_chip = jnp.where(way == 0, chips - 1 - skip, skip)
                    own = contribution(part, to_chip)

                    @pl.when(behind > 0)
                    def _():
                        held = slots[way, slot, part, :].astype(jnp.float32)
                        slots[way, slot, part, :] = (held + own).astype(jnp.bfloat16)

                    @pl.when(behind == 0)
                    def _():
                        slots[way, slot, part, :] = own.astype(jnp.bfloat16)

            loop(2, take)

            @pl.when((slot < chips - 2) | (piece < pieces - 1))
            def _():
                give(slot, piece)

        loop(pieces, piece_step)

        @pl.when(slot == 0)
        def _():
            weight_product(chip, w, True)

            def own_piece(piece):
                part = aligned(piece, piece_rows)
                own_grad[part, :] = contribution(part, chip)

            loop(pieces, own_piece)

        def use_weight(way):
            behind, _ = place(way)

            @pl.when(slot < behind)
            def _():
                from_chip = jnp.where(way == 0, chip - 1 - slot, chip + 1 + slot)
                weight_product(from_chip, slots.at[way, slot], False)

        loop(2, use_weight)

    loop(chips - 1, slot_step)

    groups = product_sem.shape[0] - 1
    group = blocks // groups

    def share_product(which, index=0):
        theirs = product.at[which, pl.ds(tokens, tokens)]
        return share(theirs, product_in.at[which], product_sem, index)

    for k in range(groups):
        share_product(pl.ds(k * group, group), k).start()

    gain_rows = rows // LANES
    half_rows = gain_parts.shape[1]
    slopes[...] = jnp.zeros_like(slopes)
    per_block = block // LANES

    def slope_sums(at):
        for k in range(per_block):
            inner = slice(k * LANES, (k + 1) * LANES)
            lanes = aligned(at * per_block + k, LANES)
            scale = gain[lanes].reshape(1, LANES)

            def some_rows(row, gain_total):
                part = aligned(row, LANES)
                value = product[at, part, inner] + product_in[at, part, inner]
                product[at, part, inner] = value
                xhat = standardized(part, lanes)
                slope = value * scale
                slopes[0, part, :] += slope
                slopes[1, part, :] += slope * xhat
                return gain_total + jnp.sum((value * xhat).reshape(-1, 8, LANES), axis=0)

            gain_total = lax.fori_loop(0, row_blocks, some_rows, jnp.zeros((8, LANES), jnp.float32))
            gain_parts[(at * per_block + k) // half_rows, pl.ds((at * per_block + k) % half_rows, 1), :] = jnp.sum(gain_total, axis=0, keepdims=True)

    for k in range(groups):
        share_product(pl.ds(k * group, group), k).wait_recv()
        loop(group, lambda at: slope_sums(k * group + at))

    for at in range(gain_rows, CORES * half_rows):
        total = jnp.sum(qk_part[...], axis=0, keepdims=True)
        row = total if at == gain_rows else jnp.zeros_like(total)
        gain_parts[at // half_rows, at % half_rows : at % half_rows + 1, :] = row

    def spread_gains(k):
        mine = gain_chips.at[chip]
        return pltpu.make_async_remote_copy(
            src_ref=mine,
            dst_ref=mine,
            send_sem=gain_sem.at[0],
            recv_sem=gain_sem.at[1],
            device_id=(lax.rem(dp + CORES * k, dp_count), mp),
            device_id_type=MESH,
        )

    first_swap = share(gain_parts.at[1 - core], gain_in, gain_sem, 1)
    first_swap.start()
    for at in range(row_blocks):
        part = slice(at * LANES, (at + 1) * LANES)
        row_sums[1, 0, at : at + 1, :] = as_row(slopes[0, part, :])
        row_sums[1, 0, row_blocks + at : row_blocks + at + 1, :] = as_row(slopes[1, part, :])
    exchange(1, 0).start()
    first_swap.wait()
    gain_chips[chip] = gain_parts[core] + gain_in[...]
    loop(chips - 1, lambda k: spread_gains(k + 1).start())
    give(chips - 2, pieces - 1)
    for stage in range(stages - 1):
        add_stage(1, stage)
    sums = add_stage(1, stages - 1)
    for at in range(row_blocks):
        part = slice(at * LANES, (at + 1) * LANES)
        slopes[0, part, :] = as_tile(sums[at : at + 1])
        slopes[1, part, :] = as_tile(sums[row_blocks + at : row_blocks + at + 1])

    def finish_rows(row):
        part = aligned(row, LANES)
        for k in range(gain_rows):
            lanes = slice(k * LANES, (k + 1) * LANES)
            at, inner = k // per_block, k % per_block * LANES
            slope = product[at, part, inner : inner + LANES] * gain[lanes].reshape(1, LANES)
            value = deviation[part, :] * (
                slope - slopes[0, part, :] - standardized(part, lanes) * slopes[1, part, :]
            )
            input_grad[part, lanes] = value.astype(jnp.bfloat16)

    loop(row_blocks, finish_rows)

    others = gain_chips.at[pl.ds(0, chips - 1)]
    for k in range(2):
        pltpu.make_async_copy(others, others, gain_sem.at[k]).wait()
    gain_totals[core] = lax.fori_loop(1, chips, lambda k, total: total + gain_chips[k], gain_chips[0])
    total = gain_totals.at[core]
    last_swap = share(total, total, gain_sem, 2)
    last_swap.start()
    last_swap.wait()
    for k in range(gain_rows):
        gain_out[k * LANES : (k + 1) * LANES] = gain_totals[k // half_rows, k % half_rows]
    qk_out[...] = gain_totals[gain_rows // half_rows, gain_rows % half_rows]

    def finish_piece(piece):
        part = aligned(piece, piece_rows)

        def one(way):
            @pl.when(place(way)[0] > 0)
            def _():
                arrival(way, chips - 1, piece).wait_recv()
                own_grad[part, :] += slots[way, chips - 1, part, :].astype(jnp.float32)

        loop(2, one)

    share_query(slice(None)).wait_send()
    share_normed(slice(None)).wait_send()
    share_product(slice(None)).wait_send()
    loop(pieces, finish_piece)
    for way in range(2):
        @pl.when(place(way)[1])
        def _():
            pltpu.make_async_copy(slots.at[way], slots.at[way], send_sem.at[way]).wait()


def write_kernel(parts, *refs):
    count = len(refs) // 2
    sources, targets, sem = refs[:count], refs[count:-1], refs[-1]
    copies = []
    for source, target in zip(sources, targets):
        pieces = parts if len(source.shape) > 1 else 1
        size = source.shape[0] // pieces
        for i in range(pieces):
            part = pl.ds(i * size, size)
            copies.append(pltpu.make_async_copy(source.at[part], target.at[part], sem.at[len(copies)]))
    for copy in copies:
        copy.start()
    for copy in copies:
        copy.wait()


def fused(block_input, prenorm_gain, weight, query, grad_normed, qk_gain):
    dp_count, mp_count = lax.axis_size("dp"), lax.axis_size("mp")
    chips = dp_count // CORES
    tokens, rows = block_input.shape
    columns = weight.shape[1]
    features = query.shape[1]
    pieces = next(count for count in (3, 2, 1) if rows // LANES % count == 0)
    block = math.gcd(rows, 2 * LANES)
    gain_rows = -(-(rows // LANES + 1) // (8 * CORES)) * 8
    stages = mp_count.bit_length() - 1
    anywhere = pl.BlockSpec(memory_space=pl.ANY)
    local = pl.BlockSpec(memory_space=pltpu.VMEM)
    bf16, f32 = jnp.bfloat16, jnp.float32
    dma = pltpu.SemaphoreType.DMA
    results = pl.pallas_call(
        functools.partial(fused_kernel, (dp_count, mp_count, pieces)),
        in_specs=[anywhere] * 6,
        out_specs=[local] * 4,
        out_shape=[
            pltpu.VMEM((tokens, rows), bf16),
            pltpu.VMEM((rows, columns), f32),
            pltpu.VMEM((rows,), f32),
            pltpu.VMEM((LANES,), f32),
        ],
        scratch_shapes=[
            pltpu.VMEM((tokens, rows), bf16),
            pltpu.VMEM((rows, columns), bf16),
            pltpu.VMEM((2, tokens, features), bf16),
            pltpu.VMEM((rows,), f32),
            pltpu.VMEM((LANES,), f32),
            pltpu.VMEM((2, chips, rows, columns), bf16),
            pltpu.VMEM((chips, CORES * tokens, columns), bf16),
            pltpu.VMEM((chips, tokens, columns), bf16),
            pltpu.VMEM((CORES, rows, tokens), bf16),
            pltpu.VMEM((rows // block, CORES * tokens, block), f32),
            pltpu.VMEM((rows // block, tokens, block), f32),
            pltpu.VMEM((tokens, LANES), f32),
            pltpu.VMEM((tokens, LANES), f32),
            pltpu.VMEM((2, tokens, LANES), f32),
            pltpu.VMEM((2, stages, 2 * tokens // LANES, LANES), f32),
            pltpu.VMEM((2, stages, 2 * tokens // LANES, LANES), f32),
            pltpu.VMEM((CORES, gain_rows, LANES), f32),
            pltpu.VMEM((gain_rows, LANES), f32),
            pltpu.VMEM((chips, gain_rows, LANES), f32),
            pltpu.VMEM((CORES, gain_rows, LANES), f32),
            pltpu.VMEM((8, LANES), f32),
            dma((4,)),
            dma((pieces,)),
            pltpu.SemaphoreType.REGULAR((2 + stages,)),
            dma((2,)),
            dma((2, chips, pieces)),
            dma((2,)),
            dma((2,)),
            dma((1 + math.gcd(rows // block, 2),)),
            dma((1 + 2 * stages,)),
            dma((4,)),
        ],
        compiler_params=pltpu.CompilerParams(
            collective_id=0, has_side_effects=True, vmem_limit_bytes=56 * 1024 * 1024
        ),
        cost_estimate=pl.CostEstimate(
            flops=8 * tokens * rows * features, bytes_accessed=8 * tokens * features, transcendentals=0
        ),
    )(block_input, prenorm_gain, weight, query, grad_normed, qk_gain)
    parts = 1
    return pl.pallas_call(
        functools.partial(write_kernel, parts),
        in_specs=[local] * 4,
        out_specs=[anywhere] * 4,
        out_shape=[jax.ShapeDtypeStruct(result.shape, result.dtype) for result in results],
        scratch_shapes=[dma((2 * parts + 2,))],
        compiler_params=pltpu.CompilerParams(vmem_limit_bytes=4 * 1024 * 1024),
    )(*[pltpu.with_memory_space_constraint(result, pltpu.VMEM) for result in results])


def shards(block_input, prenorm_gain, weight, query, grad_normed, qk_gain):
    tokens, rows = block_input.shape
    sizes = (tokens, rows, weight.shape[1])
    whole_tiles = all(size % LANES == 0 for size in sizes) and qk_gain.shape[0] == LANES
    mp_count = lax.axis_size("mp")
    several = lax.axis_size("dp") > CORES and mp_count > 1 and mp_count & (mp_count - 1) == 0
    body = fused if whole_tiles and several else permuted
    return body(block_input, prenorm_gain, weight, query, grad_normed, qk_gain)


def solution(mesh):
    return jax.shard_map(
        shards,
        mesh=mesh,
        in_specs=(P("dp", "mp"), P("mp"), P("mp", "dp"), P("dp", None), P("dp", None), P()),
        out_specs=(P("dp", "mp"), P("mp", "dp"), P("mp"), P()),
        check_vma=False,
    )
```

```python
import functools
import math

import jax
import jax.numpy as jnp
from jax import lax
from jax.experimental import pallas as pl
from jax.experimental.pallas import tpu as pltpu
from jax.sharding import PartitionSpec as P

D = 6144


EPS = 1e-06


def qk_kernel(query_ref, grad_ref, gain_ref, out_ref, contrib_ref):
    @pl.when(pl.program_id(0) == 0)
    def _():
        contrib_ref[...] = jnp.zeros_like(contrib_ref)

    head_size = gain_ref.shape[1]
    gain = gain_ref[...]
    total = jnp.zeros_like(contrib_ref)
    for head in range(query_ref.shape[1] // head_size):
        columns = pl.ds(head * head_size, head_size)
        q_float = query_ref[:, columns].astype(jnp.float32)
        upstream = grad_ref[:, columns].astype(jnp.float32)
        q_mean = jnp.mean(q_float, axis=1, keepdims=True)
        q_var = jnp.mean(q_float * q_float, axis=1, keepdims=True) - q_mean * q_mean
        q_inv = lax.rsqrt(q_var + EPS)
        qhat = (q_float - q_mean) * q_inv
        dqhat = upstream * gain
        dq_mean = jnp.mean(dqhat, axis=1, keepdims=True)
        dq_cross = jnp.mean(dqhat * qhat, axis=1, keepdims=True)
        out_ref[:, columns] = (q_inv * (dqhat - dq_mean - qhat * dq_cross)).astype(out_ref.dtype)
        product = upstream * qhat
        total += jnp.sum(product.reshape(-1, 8, head_size), axis=0)
    contrib_ref[...] += total


def qk_backward(query, grad_normed, qk_gain):
    rows, width = query.shape
    head_size = qk_gain.shape[0]
    block = min(rows, 64)
    grad_query, contrib = pl.pallas_call(
        qk_kernel,
        grid=(rows // block,),
        in_specs=[
            pl.BlockSpec((block, width), lambda i: (i, 0)),
            pl.BlockSpec((block, width), lambda i: (i, 0)),
            pl.BlockSpec((1, head_size), lambda i: (0, 0)),
        ],
        out_specs=[
            pl.BlockSpec((block, width), lambda i: (i, 0)),
            pl.BlockSpec((8, head_size), lambda i: (0, 0)),
        ],
        out_shape=[
            jax.ShapeDtypeStruct((rows, width), jnp.bfloat16),
            jax.ShapeDtypeStruct((8, head_size), jnp.float32),
        ],
        compiler_params=pltpu.CompilerParams(vmem_limit_bytes=32 * 1024 * 1024),
        cost_estimate=pl.CostEstimate(flops=40 * rows * width, bytes_accessed=6 * rows * width, transcendentals=0),
    )(query, grad_normed, qk_gain.reshape(1, -1))
    return grad_query, jnp.sum(contrib, axis=0)


CORES = 2


def line_move(value, shift, valid):
    chips = lax.axis_size("dp") // CORES
    pairs = [
        (chip * CORES + core, (chip + shift) * CORES + core)
        for chip in range(chips)
        for core in range(CORES)
        if 0 <= chip + shift < chips and valid(chip)
    ]
    return lax.ppermute(value, "dp", pairs)


def partner_swap(value):
    count = lax.axis_size("dp")
    pairs = [(at, at - at % CORES + (at + 1) % CORES) for at in range(count)]
    return lax.ppermute(value, "dp", pairs)


def add_kernel(*refs):
    total = refs[0][...]
    for ref in refs[1:-1]:
        total = total + ref[...].astype(jnp.float32)
    refs[-1][...] = total.astype(jnp.bfloat16)


def add_terms(*terms):
    rows, width = terms[0].shape
    block = math.gcd(rows, 256)
    spec = pl.BlockSpec((block, width), lambda i: (i, 0))
    return pl.pallas_call(
        add_kernel,
        grid=(rows // block,),
        in_specs=[spec] * len(terms),
        out_specs=spec,
        out_shape=jax.ShapeDtypeStruct((rows, width), jnp.bfloat16),
        compiler_params=pltpu.CompilerParams(vmem_limit_bytes=16 * 1024 * 1024),
        cost_estimate=pl.CostEstimate(
            flops=3 * rows * width, bytes_accessed=10 * rows * width, transcendentals=0
        ),
    )(*terms)


def permuted(block_input, prenorm_gain, weight, query, grad_normed, qk_gain):
    chips = lax.axis_size("dp") // CORES
    chip = lax.axis_index("dp") // CORES
    core = lax.axis_index("dp") % CORES
    columns = weight.shape[1]
    pair_columns = columns * CORES

    steps = []
    rightward, leftward = weight, weight
    for step in range(1, chips):
        rightward = line_move(rightward, 1, lambda at: at - step + 1 >= 0)
        leftward = line_move(leftward, -1, lambda at: at + step - 1 < chips)
        steps.append((rightward, leftward))

    input_wide_float = block_input.astype(jnp.float32)
    local_sum = jnp.sum(input_wide_float, axis=1)
    local_square = jnp.sum(input_wide_float * input_wide_float, axis=1)
    total_sum, total_square = lax.psum((local_sum, local_square), "mp")
    row_average = (total_sum / D)[:, None]
    reciprocal_deviation = lax.rsqrt((total_square / D)[:, None] - row_average * row_average + EPS)
    standardized_input = (input_wide_float - row_average) * reciprocal_deviation
    prenormed_rows = (standardized_input * prenorm_gain).astype(jnp.bfloat16)
    grad_query, qk_partial = qk_backward(query, grad_normed, qk_gain)

    def chip_columns(offset):
        first = lax.rem(chip + offset + chips, chips) * pair_columns
        return lax.dynamic_slice_in_dim(grad_query, first, pair_columns, 1)

    order = []
    for step in range(1, chips):
        for offset in ((chips - step) % chips, step):
            if offset not in order:
                order.append(offset)
    order.append(0)
    own, theirs = {}, {}
    for offset in order:
        part = lax.dot_general(
            prenormed_rows,
            chip_columns(offset),
            (((0,), (0,)), ((), ())),
            preferred_element_type=jnp.float32,
        )
        own[offset] = lax.dynamic_slice_in_dim(part, core * columns, columns, 1)
        theirs[offset] = partner_swap(
            lax.dynamic_slice_in_dim(part, (1 - core) * columns, columns, 1).astype(jnp.bfloat16)
        )

    to_right, to_left = None, None
    for step in range(1, chips):
        right_terms = [own[chips - step], theirs[chips - step]]
        left_terms = [own[step], theirs[step]]
        if step > 1:
            right_terms.append(to_right)
            left_terms.append(to_left)
        to_right = line_move(add_terms(*right_terms), 1, lambda at: at < step)
        to_left = line_move(add_terms(*left_terms), -1, lambda at: at >= chips - step)
    grad_weight = own[0] + theirs[0].astype(jnp.float32)
    if chips > 1:
        grad_weight = grad_weight + to_right.astype(jnp.float32) + to_left.astype(jnp.float32)

    def product(block, offset):
        other = partner_swap(block)
        first = jnp.where(core == 0, block, other)
        second = jnp.where(core == 0, other, block)
        return lax.dot_general(
            chip_columns(offset),
            jnp.concatenate([first, second], axis=1),
            (((1,), (1,)), ((), ())),
            preferred_element_type=jnp.float32,
        )

    gradient_prenormed_input = product(weight, 0)
    for step in range(1, chips):
        rightward, leftward = steps[step - 1]
        if 2 * step >= chips:
            from_left = chip >= step
            gradient_prenormed_input += product(
                jnp.where(from_left, rightward, leftward), jnp.where(from_left, -step, step)
            )
        else:
            gradient_prenormed_input += product(rightward, -step)
            gradient_prenormed_input += product(leftward, step)

    standardized_gradient = gradient_prenormed_input * prenorm_gain
    slope_mean, slope_cross = lax.psum(
        (
            jnp.sum(standardized_gradient, axis=1),
            jnp.sum(standardized_gradient * standardized_input, axis=1),
        ),
        "mp",
    )
    average_standardized_gradient = (slope_mean / D)[:, None]
    average_cross_term = (slope_cross / D)[:, None]
    input_gradient = (
        reciprocal_deviation
        * (
            standardized_gradient
            - average_standardized_gradient
            - standardized_input * average_cross_term
        )
    ).astype(jnp.bfloat16)
    prenorm_gain_partial = jnp.sum(gradient_prenormed_input * standardized_input, axis=0)
    prenorm_gain_gradient, grad_qk_gain = lax.psum((prenorm_gain_partial, qk_partial), "dp")
    return (input_gradient, grad_weight, prenorm_gain_gradient, grad_qk_gain)


LANES = 128
MESH = pl.DeviceIdType.MESH


def loop(count, body):
    def step(i, carry):
        body(i)
        return carry

    lax.fori_loop(0, count, step, 0)


def aligned(at, size):
    return pl.ds(pl.multiple_of(at * size, size), size)


def fused_kernel(
    sizes,
    x_ref,
    gain_ref,
    w_ref,
    query_ref,
    grad_ref,
    qk_gain_ref,
    input_grad,
    own_grad,
    tail,
    gain_out,
    qk_out,
    x,
    w,
    queries,
    gain,
    qk_scale,
    slots,
    grad_query,
    grad_query_out,
    normed_t,
    product,
    product_in,
    average,
    deviation,
    slopes,
    row_sums,
    row_sums_in,
    gain_parts,
    gain_in,
    gain_chips,
    gain_totals,
    qk_part,
    load_sem,
    weight_sem,
    ready_sem,
    send_sem,
    recv_sem,
    query_sem,
    normed_sem,
    product_sem,
    sums_sem,
    gain_sem,
):
    dp_count, mp_count, pieces = sizes
    chips = dp_count // CORES
    tokens, rows = x_ref.shape
    columns = w_ref.shape[1]
    piece_rows = rows // pieces
    width = rows * mp_count
    blocks, _, block = product.shape
    row_blocks = tokens // LANES
    heads = columns // LANES

    dp = lax.axis_index("dp")
    mp = lax.axis_index("mp")
    chip = dp // CORES
    core = dp % CORES
    partner = (chip * CORES + 1 - core, mp)

    stages = mp_count.bit_length() - 1

    def mp_peer(stage):
        bit = 1 << stage
        return (dp, mp + bit - 2 * bit * (mp // bit % 2))

    def load_weight(piece):
        part = aligned(piece, piece_rows)
        return pltpu.make_async_copy(w_ref.at[part], w.at[part], weight_sem.at[piece])

    loop(pieces, lambda piece: load_weight(piece).start())

    barrier = pltpu.get_barrier_semaphore()

    def place(way):
        behind = jnp.where(way == 0, chip, chips - 1 - chip)
        return behind, behind < chips - 1

    def next_chip(way):
        return (dp + CORES * (1 - 2 * way), mp)

    def tell(semaphore, peer):
        pl.semaphore_signal(semaphore, inc=1, device_id=peer, device_id_type=MESH)

    pairs = [(chip > 0, next_chip(1), chip < chips - 1, next_chip(0)), (core == 1, partner, core == 0, partner)]
    for stage in range(stages):
        low = mp // (1 << stage) % 2 == 0
        pairs.append((~low, mp_peer(stage), low, mp_peer(stage)))
    for _, _, below, peer in pairs:
        @pl.when(below)
        def _():
            tell(barrier, peer)

    above_count = sum(jnp.where(above, 1, 0) for above, _, _, _ in pairs)

    @pl.when(above_count > 0)
    def _():
        pl.semaphore_wait(barrier, above_count)

    for k, (above, peer, _, _) in enumerate(pairs):
        @pl.when(above)
        def _():
            tell(ready_sem.at[min(k, 1)], peer)

    def await_ready(group, which):
        count = sum(jnp.where(below, 1, 0) for _, _, below, _ in which)

        @pl.when(count > 0)
        def _():
            pl.semaphore_wait(ready_sem.at[group], count)

    def hop(way, slot, piece, source):
        part = aligned(piece, piece_rows)
        return pltpu.make_async_remote_copy(
            src_ref=source.at[part],
            dst_ref=slots.at[way, slot, part],
            send_sem=send_sem.at[way],
            recv_sem=recv_sem.at[way, slot, piece],
            device_id=next_chip(way),
            device_id_type=MESH,
        )

    def final_hop(way):
        part = pl.ds((pieces - 1) * piece_rows, piece_rows)
        return pltpu.make_async_remote_copy(
            src_ref=slots.at[way, chips - 2, part],
            dst_ref=tail.at[way],
            send_sem=send_sem.at[way],
            recv_sem=recv_sem.at[way, chips - 1, pieces - 1],
            device_id=next_chip(way),
            device_id_type=MESH,
        )

    def arrival(way, slot, piece):
        return hop(way, slot, piece, slots.at[way, slot])

    def send_weight(piece, way):
        @pl.when(place(way)[1])
        def _():
            hop(way, 0, piece, w).start()

    def load_and_send(piece):
        load_weight(piece).wait()
        send_weight(piece, 1)

    loop(pieces, load_and_send)
    await_ready(0, pairs[:1])
    loop(pieces, lambda piece: send_weight(piece, 0))

    loads = [
        pltpu.make_async_copy(source, target, load_sem.at[i])
        for i, (source, target) in enumerate(
            ((x_ref, x), (gain_ref, gain), (qk_gain_ref, qk_scale))
        )
    ]
    for load in loads:
        load.start()
    for k, source in enumerate((query_ref, grad_ref)):
        pltpu.make_async_copy(source, queries.at[k], load_sem.at[3]).start()

    def exchange(kind, stage):
        return pltpu.make_async_remote_copy(
            src_ref=row_sums.at[kind, stage],
            dst_ref=row_sums_in.at[kind, stage],
            send_sem=sums_sem.at[0],
            recv_sem=sums_sem.at[1 + kind * stages + stage],
            device_id=mp_peer(stage),
            device_id_type=MESH,
        )

    def add_stage(kind, stage):
        exchange(kind, stage).wait()
        total = row_sums[kind, stage] + row_sums_in[kind, stage]
        if stage + 1 == stages:
            return total * (1.0 / width)
        row_sums[kind, stage + 1] = total
        exchange(kind, stage + 1).start()

    diagonal = lax.broadcasted_iota(jnp.int32, (LANES, LANES), 0) == lax.broadcasted_iota(
        jnp.int32, (LANES, LANES), 1
    )

    def as_row(tile):
        total = jnp.sum(tile, axis=1, keepdims=True)
        return jnp.sum(jnp.where(diagonal, total, 0.0), axis=0, keepdims=True)

    def as_tile(row):
        total = jnp.sum(jnp.where(diagonal, row, 0.0), axis=1, keepdims=True)
        return jnp.broadcast_to(total, (LANES, LANES))

    loads[0].wait()

    def input_sums(at):
        part = aligned(at, LANES)
        total = jnp.zeros((LANES, LANES), jnp.float32)
        square = jnp.zeros((LANES, LANES), jnp.float32)
        for k in range(rows // LANES):
            value = x[part, k * LANES : (k + 1) * LANES].astype(jnp.float32)
            total += value
            square += value * value
        row_sums[0, 0, pl.ds(at, 1), :] = as_row(total)
        row_sums[0, 0, pl.ds(row_blocks + at, 1), :] = as_row(square)

    loop(row_blocks, input_sums)
    await_ready(1, pairs[1:])
    exchange(0, 0).start()

    for load in loads[1:]:
        load.wait()
    pltpu.make_async_copy(queries, queries, load_sem.at[3]).wait()
    qk_gain = qk_scale[...].reshape(1, LANES)
    qk_part[...] = jnp.zeros_like(qk_part)
    chunk = 64

    def qk_columns(to_chip, half, target):
        first = (to_chip * CORES + half) * columns

        def some_rows(at):
            part = aligned(at, chunk)
            total = jnp.zeros_like(qk_part)
            for head in range(heads):
                lanes = pl.ds(pl.multiple_of(first + head * LANES, LANES), LANES)
                q_float = queries[0, part, lanes].astype(jnp.float32)
                upstream = queries[1, part, lanes].astype(jnp.float32)
                q_mean = jnp.mean(q_float, axis=1, keepdims=True)
                q_var = jnp.mean(q_float * q_float, axis=1, keepdims=True) - q_mean * q_mean
                q_inv = lax.rsqrt(q_var + EPS)
                qhat = (q_float - q_mean) * q_inv
                dqhat = upstream * qk_gain
                dq_mean = jnp.mean(dqhat, axis=1, keepdims=True)
                dq_cross = jnp.mean(dqhat * qhat, axis=1, keepdims=True)
                out = q_inv * (dqhat - dq_mean - qhat * dq_cross)
                target[to_chip, part, head * LANES : (head + 1) * LANES] = out.astype(jnp.bfloat16)
                total += jnp.sum((upstream * qhat).reshape(-1, 8, LANES), axis=0)
            qk_part[...] += total

        loop(tokens // chunk, some_rows)

    def share(source, target, sem, index=0):
        return pltpu.make_async_remote_copy(
            src_ref=source,
            dst_ref=target,
            send_sem=sem.at[0],
            recv_sem=sem.at[1 + index],
            device_id=partner,
            device_id_type=MESH,
        )

    def share_query(which):
        return share(grad_query_out.at[which], grad_query.at[which, pl.ds(tokens, tokens)], query_sem)

    def partner_columns(to_chip):
        qk_columns(to_chip, 1 - core, grad_query_out)
        share_query(to_chip).start()

    loop(chips, partner_columns)
    for stage in range(stages - 1):
        add_stage(0, stage)
    loop(chips, lambda to_chip: qk_columns(to_chip, core, grad_query))

    sums = add_stage(0, stages - 1)
    means = sums[:row_blocks]
    scales = lax.rsqrt(sums[row_blocks:] - means * means + EPS)
    for at in range(row_blocks):
        average[at * LANES : (at + 1) * LANES, :] = as_tile(means[at : at + 1])
        deviation[at * LANES : (at + 1) * LANES, :] = as_tile(scales[at : at + 1])

    def standardized(part, lanes):
        return (x[part, lanes].astype(jnp.float32) - average[part, :]) * deviation[part, :]

    def share_normed(part):
        return share(normed_t.at[0, part], normed_t.at[1, part], normed_sem)

    def normalize(piece):
        def some_lanes(k):
            lanes = aligned(piece * (piece_rows // LANES) + k, LANES)
            scale = gain[lanes].reshape(1, LANES)
            for at in range(row_blocks):
                part = slice(at * LANES, (at + 1) * LANES)
                value = standardized(part, lanes) * scale
                normed_t[0, lanes, part] = value.T.astype(jnp.bfloat16)

        loop(piece_rows // LANES, some_lanes)
        share_normed(aligned(piece, piece_rows)).start()

    loop(pieces, normalize)

    share_query(slice(None)).wait_recv()
    share_normed(slice(None)).wait_recv()

    def contribution(part, to_chip):
        def half(which):
            return jnp.dot(
                normed_t[which, part, :],
                grad_query[to_chip, which * tokens : (which + 1) * tokens, :],
                preferred_element_type=jnp.float32,
            )

        return half(0) + half(1)

    group = blocks // pieces
    last_weight = jnp.maximum(chip, chips - 1 - chip) - 1

    def weight_product(from_chip, weight, piece, first):
        def some_rows(k):
            at = piece * group + k
            value = lax.dot_general(
                grad_query[from_chip],
                weight[aligned(at, block), :],
                (((1,), (1,)), ((), ())),
                preferred_element_type=jnp.float32,
            )
            if first:
                product[at] = value
            else:
                product[at] += value

        loop(group, some_rows)

    def share_product(which, index=0):
        theirs = product.at[which, pl.ds(tokens, tokens)]
        return share(theirs, product_in.at[which], product_sem, index)

    def give(slot, piece):
        def one(way):
            @pl.when(place(way)[1])
            def _():
                hop(way, slot + 1, piece, slots.at[way, slot]).start()

        loop(2, one)

    def slot_step(slot):
        def piece_step(piece):
            part = aligned(piece, piece_rows)

            def take(way):
                behind, ahead = place(way)

                @pl.when(behind > 0)
                def _():
                    arrival(way, slot, piece).wait_recv()

                @pl.when(ahead & (slot >= behind))
                def _():
                    skip = slot - behind
                    to_chip = jnp.where(way == 0, chips - 1 - skip, skip)
                    own = contribution(part, to_chip)

                    @pl.when(behind > 0)
                    def _():
                        held = slots[way, slot, part, :].astype(jnp.float32)
                        slots[way, slot, part, :] = (held + own).astype(jnp.bfloat16)

                    @pl.when(behind == 0)
                    def _():
                        slots[way, slot, part, :] = own.astype(jnp.bfloat16)

            loop(2, take)

            @pl.when((slot < chips - 2) | (piece < pieces - 1))
            def _():
                give(slot, piece)

            @pl.when(slot == 0)
            def _():
                weight_product(chip, w, piece, True)
                own_grad[part, :] = contribution(part, chip)

            def use_weight(way):
                behind, _ = place(way)

                @pl.when(slot < behind)
                def _():
                    from_chip = jnp.where(way == 0, chip - 1 - slot, chip + 1 + slot)
                    weight_product(from_chip, slots.at[way, slot], piece, False)

            loop(2, use_weight)

            @pl.when(slot == last_weight)
            def _():
                share_product(aligned(piece, group), piece).start()

        loop(pieces, piece_step)

    loop(chips - 1, slot_step)

    gain_rows = rows // LANES
    half_rows = gain_parts.shape[1]
    slopes[...] = jnp.zeros_like(slopes)
    per_block = block // LANES

    def slope_sums(at):
        for k in range(per_block):
            inner = slice(k * LANES, (k + 1) * LANES)
            lanes = aligned(at * per_block + k, LANES)
            scale = gain[lanes].reshape(1, LANES)

            def some_rows(row, gain_total):
                part = aligned(row, LANES)
                value = product[at, part, inner] + product_in[at, part, inner]
                product[at, part, inner] = value
                xhat = standardized(part, lanes)
                slope = value * scale
                slopes[0, part, :] += slope
                slopes[1, part, :] += slope * xhat
                return gain_total + jnp.sum((value * xhat).reshape(-1, 8, LANES), axis=0)

            gain_total = lax.fori_loop(0, row_blocks, some_rows, jnp.zeros((8, LANES), jnp.float32))
            gain_parts[(at * per_block + k) // half_rows, pl.ds((at * per_block + k) % half_rows, 1), :] = jnp.sum(gain_total, axis=0, keepdims=True)

    for k in range(pieces):
        share_product(pl.ds(k * group, group), k).wait_recv()
        loop(group, lambda at: slope_sums(k * group + at))

    for at in range(gain_rows, CORES * half_rows):
        total = jnp.sum(qk_part[...], axis=0, keepdims=True)
        row = total if at == gain_rows else jnp.zeros_like(total)
        gain_parts[at // half_rows, at % half_rows : at % half_rows + 1, :] = row

    def spread_gains(k):
        mine = gain_chips.at[chip]
        return pltpu.make_async_remote_copy(
            src_ref=mine,
            dst_ref=mine,
            send_sem=gain_sem.at[0],
            recv_sem=gain_sem.at[1],
            device_id=(lax.rem(dp + CORES * k, dp_count), mp),
            device_id_type=MESH,
        )

    first_swap = share(gain_parts.at[1 - core], gain_in, gain_sem, 1)
    first_swap.start()
    for at in range(row_blocks):
        part = slice(at * LANES, (at + 1) * LANES)
        row_sums[1, 0, at : at + 1, :] = as_row(slopes[0, part, :])
        row_sums[1, 0, row_blocks + at : row_blocks + at + 1, :] = as_row(slopes[1, part, :])
    exchange(1, 0).start()
    first_swap.wait()
    gain_chips[chip] = gain_parts[core] + gain_in[...]
    loop(chips - 1, lambda k: spread_gains(k + 1).start())
    for way in range(2):
        @pl.when(place(way)[1])
        def _():
            final_hop(way).start()

    for stage in range(stages - 1):
        add_stage(1, stage)
    sums = add_stage(1, stages - 1)
    for at in range(row_blocks):
        part = slice(at * LANES, (at + 1) * LANES)
        slopes[0, part, :] = as_tile(sums[at : at + 1])
        slopes[1, part, :] = as_tile(sums[row_blocks + at : row_blocks + at + 1])

    def finish_rows(row):
        part = aligned(row, LANES)
        for k in range(gain_rows):
            lanes = slice(k * LANES, (k + 1) * LANES)
            at, inner = k // per_block, k % per_block * LANES
            slope = product[at, part, inner : inner + LANES] * gain[lanes].reshape(1, LANES)
            value = deviation[part, :] * (
                slope - slopes[0, part, :] - standardized(part, lanes) * slopes[1, part, :]
            )
            input_grad[part, lanes] = value.astype(jnp.bfloat16)

    loop(row_blocks, finish_rows)

    others = gain_chips.at[pl.ds(0, chips - 1)]
    for k in range(2):
        pltpu.make_async_copy(others, others, gain_sem.at[k]).wait()
    gain_totals[core] = lax.fori_loop(1, chips, lambda k, total: total + gain_chips[k], gain_chips[0])
    total = gain_totals.at[core]
    last_swap = share(total, total, gain_sem, 2)
    last_swap.start()
    last_swap.wait()
    for k in range(gain_rows):
        gain_out[k * LANES : (k + 1) * LANES] = gain_totals[k // half_rows, k % half_rows]
    qk_out[...] = gain_totals[gain_rows // half_rows, gain_rows % half_rows]

    def finish_piece(piece):
        part = aligned(piece, piece_rows)

        def one(way):
            @pl.when(place(way)[0] > 0)
            def _():
                arrival(way, chips - 1, piece).wait_recv()
                own_grad[part, :] += slots[way, chips - 1, part, :].astype(jnp.float32)

        loop(2, one)

    share_query(slice(None)).wait_send()
    share_normed(slice(None)).wait_send()
    share_product(slice(None)).wait_send()
    loop(pieces - 1, finish_piece)
    for way in range(2):
        @pl.when(place(way)[0] > 0)
        def _():
            final_hop(way).wait_recv()

    for way in range(2):
        @pl.when(place(way)[1])
        def _():
            pltpu.make_async_copy(slots.at[way], slots.at[way], send_sem.at[way]).wait()


def write_kernel(input_grad, own_grad, tail, gain, qk, input_ref, weight_ref, gain_ref, qk_ref, last, sem):
    rows = own_grad.shape[0]
    most = rows - last.shape[0]
    copies = [
        pltpu.make_async_copy(own_grad.at[pl.ds(0, most)], weight_ref.at[pl.ds(0, most)], sem.at[0]),
        pltpu.make_async_copy(input_grad, input_ref, sem.at[1]),
        pltpu.make_async_copy(gain, gain_ref, sem.at[2]),
        pltpu.make_async_copy(qk, qk_ref, sem.at[3]),
        pltpu.make_async_copy(last, weight_ref.at[pl.ds(most, rows - most)], sem.at[4]),
    ]
    for copy in copies[:-1]:
        copy.start()
    chips = lax.axis_size("dp") // CORES
    chip = lax.axis_index("dp") // CORES
    last[...] = own_grad[most:, :]
    for way, receives in enumerate((chip > 0, chip < chips - 1)):
        @pl.when(receives)
        def _():
            last[...] += tail[way].astype(jnp.float32)

    copies[-1].start()
    for copy in copies:
        copy.wait()


def fused(block_input, prenorm_gain, weight, query, grad_normed, qk_gain):
    dp_count, mp_count = lax.axis_size("dp"), lax.axis_size("mp")
    chips = dp_count // CORES
    tokens, rows = block_input.shape
    columns = weight.shape[1]
    features = query.shape[1]
    pieces = next(count for count in (3, 2, 1) if rows // LANES % count == 0)
    block = math.gcd(rows // pieces, 2 * LANES)
    gain_rows = -(-(rows // LANES + 1) // (8 * CORES)) * 8
    stages = mp_count.bit_length() - 1
    anywhere = pl.BlockSpec(memory_space=pl.ANY)
    local = pl.BlockSpec(memory_space=pltpu.VMEM)
    bf16, f32 = jnp.bfloat16, jnp.float32
    dma = pltpu.SemaphoreType.DMA
    results = pl.pallas_call(
        functools.partial(fused_kernel, (dp_count, mp_count, pieces)),
        in_specs=[anywhere] * 6,
        out_specs=[local] * 5,
        out_shape=[
            pltpu.VMEM((tokens, rows), bf16),
            pltpu.VMEM((rows, columns), f32),
            pltpu.VMEM((2, rows // pieces, columns), bf16),
            pltpu.VMEM((rows,), f32),
            pltpu.VMEM((LANES,), f32),
        ],
        scratch_shapes=[
            pltpu.VMEM((tokens, rows), bf16),
            pltpu.VMEM((rows, columns), bf16),
            pltpu.VMEM((2, tokens, features), bf16),
            pltpu.VMEM((rows,), f32),
            pltpu.VMEM((LANES,), f32),
            pltpu.VMEM((2, chips, rows, columns), bf16),
            pltpu.VMEM((chips, CORES * tokens, columns), bf16),
            pltpu.VMEM((chips, tokens, columns), bf16),
            pltpu.VMEM((CORES, rows, tokens), bf16),
            pltpu.VMEM((rows // block, CORES * tokens, block), f32),
            pltpu.VMEM((rows // block, tokens, block), f32),
            pltpu.VMEM((tokens, LANES), f32),
            pltpu.VMEM((tokens, LANES), f32),
            pltpu.VMEM((2, tokens, LANES), f32),
            pltpu.VMEM((2, stages, 2 * tokens // LANES, LANES), f32),
            pltpu.VMEM((2, stages, 2 * tokens // LANES, LANES), f32),
            pltpu.VMEM((CORES, gain_rows, LANES), f32),
            pltpu.VMEM((gain_rows, LANES), f32),
            pltpu.VMEM((chips, gain_rows, LANES), f32),
            pltpu.VMEM((CORES, gain_rows, LANES), f32),
            pltpu.VMEM((8, LANES), f32),
            dma((4,)),
            dma((pieces,)),
            pltpu.SemaphoreType.REGULAR((2,)),
            dma((2,)),
            dma((2, chips, pieces)),
            dma((2,)),
            dma((2,)),
            dma((1 + pieces,)),
            dma((1 + 2 * stages,)),
            dma((4,)),
        ],
        compiler_params=pltpu.CompilerParams(
            collective_id=0, has_side_effects=True, vmem_limit_bytes=56 * 1024 * 1024
        ),
        cost_estimate=pl.CostEstimate(
            flops=8 * tokens * rows * features, bytes_accessed=8 * tokens * features, transcendentals=0
        ),
    )(block_input, prenorm_gain, weight, query, grad_normed, qk_gain)
    outputs = [results[0], results[1], results[3], results[4]]
    return pl.pallas_call(
        write_kernel,
        in_specs=[local] * 5,
        out_specs=[anywhere] * 4,
        out_shape=[jax.ShapeDtypeStruct(output.shape, output.dtype) for output in outputs],
        scratch_shapes=[pltpu.VMEM((rows // pieces, columns), f32), dma((5,))],
        compiler_params=pltpu.CompilerParams(vmem_limit_bytes=4 * 1024 * 1024),
    )(*[pltpu.with_memory_space_constraint(result, pltpu.VMEM) for result in results])


def shards(block_input, prenorm_gain, weight, query, grad_normed, qk_gain):
    tokens, rows = block_input.shape
    sizes = (tokens, rows, weight.shape[1])
    whole_tiles = all(size % LANES == 0 for size in sizes) and qk_gain.shape[0] == LANES
    mp_count = lax.axis_size("mp")
    several = lax.axis_size("dp") > CORES and mp_count > 1 and mp_count & (mp_count - 1) == 0
    body = fused if whole_tiles and several else permuted
    return body(block_input, prenorm_gain, weight, query, grad_normed, qk_gain)


def solution(mesh):
    return jax.shard_map(
        shards,
        mesh=mesh,
        in_specs=(P("dp", "mp"), P("mp"), P("mp", "dp"), P("dp", None), P("dp", None), P()),
        out_specs=(P("dp", "mp"), P("mp", "dp"), P("mp"), P()),
        check_vma=False,
    )
```

```python
import functools
import math

import jax
import jax.numpy as jnp
from jax import lax
from jax.experimental import pallas as pl
from jax.experimental.pallas import tpu as pltpu
from jax.sharding import PartitionSpec as P

D = 6144


EPS = 1e-06


def qk_kernel(query_ref, grad_ref, gain_ref, out_ref, contrib_ref):
    @pl.when(pl.program_id(0) == 0)
    def _():
        contrib_ref[...] = jnp.zeros_like(contrib_ref)

    head_size = gain_ref.shape[1]
    gain = gain_ref[...]
    total = jnp.zeros_like(contrib_ref)
    for head in range(query_ref.shape[1] // head_size):
        columns = pl.ds(head * head_size, head_size)
        q_float = query_ref[:, columns].astype(jnp.float32)
        upstream = grad_ref[:, columns].astype(jnp.float32)
        q_mean = jnp.mean(q_float, axis=1, keepdims=True)
        q_var = jnp.mean(q_float * q_float, axis=1, keepdims=True) - q_mean * q_mean
        q_inv = lax.rsqrt(q_var + EPS)
        qhat = (q_float - q_mean) * q_inv
        dqhat = upstream * gain
        dq_mean = jnp.mean(dqhat, axis=1, keepdims=True)
        dq_cross = jnp.mean(dqhat * qhat, axis=1, keepdims=True)
        out_ref[:, columns] = (q_inv * (dqhat - dq_mean - qhat * dq_cross)).astype(out_ref.dtype)
        product = upstream * qhat
        total += jnp.sum(product.reshape(-1, 8, head_size), axis=0)
    contrib_ref[...] += total


def qk_backward(query, grad_normed, qk_gain):
    rows, width = query.shape
    head_size = qk_gain.shape[0]
    block = min(rows, 64)
    grad_query, contrib = pl.pallas_call(
        qk_kernel,
        grid=(rows // block,),
        in_specs=[
            pl.BlockSpec((block, width), lambda i: (i, 0)),
            pl.BlockSpec((block, width), lambda i: (i, 0)),
            pl.BlockSpec((1, head_size), lambda i: (0, 0)),
        ],
        out_specs=[
            pl.BlockSpec((block, width), lambda i: (i, 0)),
            pl.BlockSpec((8, head_size), lambda i: (0, 0)),
        ],
        out_shape=[
            jax.ShapeDtypeStruct((rows, width), jnp.bfloat16),
            jax.ShapeDtypeStruct((8, head_size), jnp.float32),
        ],
        compiler_params=pltpu.CompilerParams(vmem_limit_bytes=32 * 1024 * 1024),
        cost_estimate=pl.CostEstimate(flops=40 * rows * width, bytes_accessed=6 * rows * width, transcendentals=0),
    )(query, grad_normed, qk_gain.reshape(1, -1))
    return grad_query, jnp.sum(contrib, axis=0)


CORES = 2


def line_move(value, shift, valid):
    chips = lax.axis_size("dp") // CORES
    pairs = [
        (chip * CORES + core, (chip + shift) * CORES + core)
        for chip in range(chips)
        for core in range(CORES)
        if 0 <= chip + shift < chips and valid(chip)
    ]
    return lax.ppermute(value, "dp", pairs)


def partner_swap(value):
    count = lax.axis_size("dp")
    pairs = [(at, at - at % CORES + (at + 1) % CORES) for at in range(count)]
    return lax.ppermute(value, "dp", pairs)


def add_kernel(*refs):
    total = refs[0][...]
    for ref in refs[1:-1]:
        total = total + ref[...].astype(jnp.float32)
    refs[-1][...] = total.astype(jnp.bfloat16)


def add_terms(*terms):
    rows, width = terms[0].shape
    block = math.gcd(rows, 256)
    spec = pl.BlockSpec((block, width), lambda i: (i, 0))
    return pl.pallas_call(
        add_kernel,
        grid=(rows // block,),
        in_specs=[spec] * len(terms),
        out_specs=spec,
        out_shape=jax.ShapeDtypeStruct((rows, width), jnp.bfloat16),
        compiler_params=pltpu.CompilerParams(vmem_limit_bytes=16 * 1024 * 1024),
        cost_estimate=pl.CostEstimate(
            flops=3 * rows * width, bytes_accessed=10 * rows * width, transcendentals=0
        ),
    )(*terms)


def permuted(block_input, prenorm_gain, weight, query, grad_normed, qk_gain):
    chips = lax.axis_size("dp") // CORES
    chip = lax.axis_index("dp") // CORES
    core = lax.axis_index("dp") % CORES
    columns = weight.shape[1]
    pair_columns = columns * CORES

    steps = []
    rightward, leftward = weight, weight
    for step in range(1, chips):
        rightward = line_move(rightward, 1, lambda at: at - step + 1 >= 0)
        leftward = line_move(leftward, -1, lambda at: at + step - 1 < chips)
        steps.append((rightward, leftward))

    input_wide_float = block_input.astype(jnp.float32)
    local_sum = jnp.sum(input_wide_float, axis=1)
    local_square = jnp.sum(input_wide_float * input_wide_float, axis=1)
    total_sum, total_square = lax.psum((local_sum, local_square), "mp")
    row_average = (total_sum / D)[:, None]
    reciprocal_deviation = lax.rsqrt((total_square / D)[:, None] - row_average * row_average + EPS)
    standardized_input = (input_wide_float - row_average) * reciprocal_deviation
    prenormed_rows = (standardized_input * prenorm_gain).astype(jnp.bfloat16)
    grad_query, qk_partial = qk_backward(query, grad_normed, qk_gain)

    def chip_columns(offset):
        first = lax.rem(chip + offset + chips, chips) * pair_columns
        return lax.dynamic_slice_in_dim(grad_query, first, pair_columns, 1)

    order = []
    for step in range(1, chips):
        for offset in ((chips - step) % chips, step):
            if offset not in order:
                order.append(offset)
    order.append(0)
    own, theirs = {}, {}
    for offset in order:
        part = lax.dot_general(
            prenormed_rows,
            chip_columns(offset),
            (((0,), (0,)), ((), ())),
            preferred_element_type=jnp.float32,
        )
        own[offset] = lax.dynamic_slice_in_dim(part, core * columns, columns, 1)
        theirs[offset] = partner_swap(
            lax.dynamic_slice_in_dim(part, (1 - core) * columns, columns, 1).astype(jnp.bfloat16)
        )

    to_right, to_left = None, None
    for step in range(1, chips):
        right_terms = [own[chips - step], theirs[chips - step]]
        left_terms = [own[step], theirs[step]]
        if step > 1:
            right_terms.append(to_right)
            left_terms.append(to_left)
        to_right = line_move(add_terms(*right_terms), 1, lambda at: at < step)
        to_left = line_move(add_terms(*left_terms), -1, lambda at: at >= chips - step)
    grad_weight = own[0] + theirs[0].astype(jnp.float32)
    if chips > 1:
        grad_weight = grad_weight + to_right.astype(jnp.float32) + to_left.astype(jnp.float32)

    def product(block, offset):
        other = partner_swap(block)
        first = jnp.where(core == 0, block, other)
        second = jnp.where(core == 0, other, block)
        return lax.dot_general(
            chip_columns(offset),
            jnp.concatenate([first, second], axis=1),
            (((1,), (1,)), ((), ())),
            preferred_element_type=jnp.float32,
        )

    gradient_prenormed_input = product(weight, 0)
    for step in range(1, chips):
        rightward, leftward = steps[step - 1]
        if 2 * step >= chips:
            from_left = chip >= step
            gradient_prenormed_input += product(
                jnp.where(from_left, rightward, leftward), jnp.where(from_left, -step, step)
            )
        else:
            gradient_prenormed_input += product(rightward, -step)
            gradient_prenormed_input += product(leftward, step)

    standardized_gradient = gradient_prenormed_input * prenorm_gain
    slope_mean, slope_cross = lax.psum(
        (
            jnp.sum(standardized_gradient, axis=1),
            jnp.sum(standardized_gradient * standardized_input, axis=1),
        ),
        "mp",
    )
    average_standardized_gradient = (slope_mean / D)[:, None]
    average_cross_term = (slope_cross / D)[:, None]
    input_gradient = (
        reciprocal_deviation
        * (
            standardized_gradient
            - average_standardized_gradient
            - standardized_input * average_cross_term
        )
    ).astype(jnp.bfloat16)
    prenorm_gain_partial = jnp.sum(gradient_prenormed_input * standardized_input, axis=0)
    prenorm_gain_gradient, grad_qk_gain = lax.psum((prenorm_gain_partial, qk_partial), "dp")
    return (input_gradient, grad_weight, prenorm_gain_gradient, grad_qk_gain)


LANES = 128
MESH = pl.DeviceIdType.MESH


def loop(count, body):
    def step(i, carry):
        body(i)
        return carry

    lax.fori_loop(0, count, step, 0)


def aligned(at, size):
    return pl.ds(pl.multiple_of(at * size, size), size)


def fused_kernel(
    sizes,
    x_ref,
    gain_ref,
    w_ref,
    query_ref,
    grad_ref,
    qk_gain_ref,
    input_grad,
    own_grad,
    tail,
    gain_out,
    qk_out,
    x,
    w,
    queries,
    gain,
    qk_scale,
    slots,
    grad_query,
    grad_query_out,
    normed_t,
    product,
    product_in,
    average,
    deviation,
    slopes,
    row_sums,
    row_sums_in,
    gain_parts,
    gain_in,
    gain_chips,
    gain_totals,
    qk_part,
    load_sem,
    weight_sem,
    ready_sem,
    send_sem,
    recv_sem,
    query_sem,
    normed_sem,
    product_sem,
    sums_sem,
    gain_sem,
):
    dp_count, mp_count, pieces = sizes
    chips = dp_count // CORES
    tokens, rows = x_ref.shape
    columns = w_ref.shape[1]
    piece_rows = rows // pieces
    width = rows * mp_count
    blocks, _, block = product.shape
    row_blocks = tokens // LANES
    heads = columns // LANES

    dp = lax.axis_index("dp")
    mp = lax.axis_index("mp")
    chip = dp // CORES
    core = dp % CORES
    partner = (chip * CORES + 1 - core, mp)

    stages = mp_count.bit_length() - 1

    def mp_peer(stage):
        bit = 1 << stage
        return (dp, mp + bit - 2 * bit * (mp // bit % 2))

    def load_weight(piece):
        part = aligned(piece, piece_rows)
        return pltpu.make_async_copy(w_ref.at[part], w.at[part], weight_sem.at[piece])

    loop(pieces, lambda piece: load_weight(piece).start())

    barrier = pltpu.get_barrier_semaphore()

    def place(way):
        behind = jnp.where(way == 0, chip, chips - 1 - chip)
        return behind, behind < chips - 1

    def next_chip(way):
        return (dp + CORES * (1 - 2 * way), mp)

    def tell(semaphore, peer):
        pl.semaphore_signal(semaphore, inc=1, device_id=peer, device_id_type=MESH)

    pairs = [(chip > 0, next_chip(1), chip < chips - 1, next_chip(0)), (core == 1, partner, core == 0, partner)]
    for stage in range(stages):
        low = mp // (1 << stage) % 2 == 0
        pairs.append((~low, mp_peer(stage), low, mp_peer(stage)))
    for _, _, below, peer in pairs:
        @pl.when(below)
        def _():
            tell(barrier, peer)

    above_count = sum(jnp.where(above, 1, 0) for above, _, _, _ in pairs)

    @pl.when(above_count > 0)
    def _():
        pl.semaphore_wait(barrier, above_count)

    for k, (above, peer, _, _) in enumerate(pairs):
        @pl.when(above)
        def _():
            tell(ready_sem.at[min(k, 1)], peer)

    def await_ready(group, which):
        count = sum(jnp.where(below, 1, 0) for _, _, below, _ in which)

        @pl.when(count > 0)
        def _():
            pl.semaphore_wait(ready_sem.at[group], count)

    def queue_of(slot, piece):
        late = jnp.where(slot == chips - 1, 1, 0)
        return late + late * jnp.where(piece == pieces - 2, 1, 0)

    def hop(way, slot, piece, source):
        part = aligned(piece, piece_rows)
        return pltpu.make_async_remote_copy(
            src_ref=source.at[part],
            dst_ref=slots.at[way, slot, part],
            send_sem=send_sem.at[queue_of(slot, piece), way],
            recv_sem=recv_sem.at[way, slot, piece],
            device_id=next_chip(way),
            device_id_type=MESH,
        )

    def final_hop(way):
        part = pl.ds((pieces - 1) * piece_rows, piece_rows)
        return pltpu.make_async_remote_copy(
            src_ref=slots.at[way, chips - 2, part],
            dst_ref=tail.at[way],
            send_sem=send_sem.at[1, way],
            recv_sem=recv_sem.at[way, chips - 1, pieces - 1],
            device_id=next_chip(way),
            device_id_type=MESH,
        )

    def arrival(way, slot, piece):
        return hop(way, slot, piece, slots.at[way, slot])

    def send_weight(piece, way):
        @pl.when(place(way)[1])
        def _():
            hop(way, 0, piece, w).start()

    def load_and_send(piece):
        load_weight(piece).wait()
        send_weight(piece, 1)

    loop(pieces, load_and_send)
    await_ready(0, pairs[:1])
    loop(pieces, lambda piece: send_weight(piece, 0))

    loads = [
        pltpu.make_async_copy(source, target, load_sem.at[i])
        for i, (source, target) in enumerate(
            ((x_ref, x), (gain_ref, gain), (qk_gain_ref, qk_scale))
        )
    ]
    for load in loads:
        load.start()
    for k, source in enumerate((query_ref, grad_ref)):
        pltpu.make_async_copy(source, queries.at[k], load_sem.at[3]).start()

    def exchange(kind, stage):
        return pltpu.make_async_remote_copy(
            src_ref=row_sums.at[kind, stage],
            dst_ref=row_sums_in.at[kind, stage],
            send_sem=sums_sem.at[0],
            recv_sem=sums_sem.at[1 + kind * stages + stage],
            device_id=mp_peer(stage),
            device_id_type=MESH,
        )

    def add_stage(kind, stage):
        exchange(kind, stage).wait()
        total = row_sums[kind, stage] + row_sums_in[kind, stage]
        if stage + 1 == stages:
            return total * (1.0 / width)
        row_sums[kind, stage + 1] = total
        exchange(kind, stage + 1).start()

    diagonal = lax.broadcasted_iota(jnp.int32, (LANES, LANES), 0) == lax.broadcasted_iota(
        jnp.int32, (LANES, LANES), 1
    )

    def as_row(tile):
        total = jnp.sum(tile, axis=1, keepdims=True)
        return jnp.sum(jnp.where(diagonal, total, 0.0), axis=0, keepdims=True)

    def as_tile(row):
        total = jnp.sum(jnp.where(diagonal, row, 0.0), axis=1, keepdims=True)
        return jnp.broadcast_to(total, (LANES, LANES))

    loads[0].wait()

    def input_sums(at):
        part = aligned(at, LANES)
        total = jnp.zeros((LANES, LANES), jnp.float32)
        square = jnp.zeros((LANES, LANES), jnp.float32)
        for k in range(rows // LANES):
            value = x[part, k * LANES : (k + 1) * LANES].astype(jnp.float32)
            total += value
            square += value * value
        row_sums[0, 0, pl.ds(at, 1), :] = as_row(total)
        row_sums[0, 0, pl.ds(row_blocks + at, 1), :] = as_row(square)

    loop(row_blocks, input_sums)
    await_ready(1, pairs[1:])
    exchange(0, 0).start()

    for load in loads[1:]:
        load.wait()
    pltpu.make_async_copy(queries, queries, load_sem.at[3]).wait()
    qk_gain = qk_scale[...].reshape(1, LANES)
    qk_part[...] = jnp.zeros_like(qk_part)
    chunk = 64

    def qk_columns(to_chip, half, target):
        first = (to_chip * CORES + half) * columns

        def some_rows(at):
            part = aligned(at, chunk)
            total = jnp.zeros_like(qk_part)
            for head in range(heads):
                lanes = pl.ds(pl.multiple_of(first + head * LANES, LANES), LANES)
                q_float = queries[0, part, lanes].astype(jnp.float32)
                upstream = queries[1, part, lanes].astype(jnp.float32)
                q_mean = jnp.mean(q_float, axis=1, keepdims=True)
                q_var = jnp.mean(q_float * q_float, axis=1, keepdims=True) - q_mean * q_mean
                q_inv = lax.rsqrt(q_var + EPS)
                qhat = (q_float - q_mean) * q_inv
                dqhat = upstream * qk_gain
                dq_mean = jnp.mean(dqhat, axis=1, keepdims=True)
                dq_cross = jnp.mean(dqhat * qhat, axis=1, keepdims=True)
                out = q_inv * (dqhat - dq_mean - qhat * dq_cross)
                target[to_chip, part, head * LANES : (head + 1) * LANES] = out.astype(jnp.bfloat16)
                total += jnp.sum((upstream * qhat).reshape(-1, 8, LANES), axis=0)
            qk_part[...] += total

        loop(tokens // chunk, some_rows)

    def share(source, target, sem, index=0):
        return pltpu.make_async_remote_copy(
            src_ref=source,
            dst_ref=target,
            send_sem=sem.at[0],
            recv_sem=sem.at[1 + index],
            device_id=partner,
            device_id_type=MESH,
        )

    def share_query(which):
        return share(grad_query_out.at[which], grad_query.at[which, pl.ds(tokens, tokens)], query_sem)

    def partner_columns(to_chip):
        qk_columns(to_chip, 1 - core, grad_query_out)
        share_query(to_chip).start()

    loop(chips, partner_columns)
    for stage in range(stages - 1):
        add_stage(0, stage)
    loop(chips, lambda to_chip: qk_columns(to_chip, core, grad_query))

    sums = add_stage(0, stages - 1)
    means = sums[:row_blocks]
    scales = lax.rsqrt(sums[row_blocks:] - means * means + EPS)
    for at in range(row_blocks):
        average[at * LANES : (at + 1) * LANES, :] = as_tile(means[at : at + 1])
        deviation[at * LANES : (at + 1) * LANES, :] = as_tile(scales[at : at + 1])

    def standardized(part, lanes):
        return (x[part, lanes].astype(jnp.float32) - average[part, :]) * deviation[part, :]

    def share_normed(part):
        return share(normed_t.at[0, part], normed_t.at[1, part], normed_sem)

    def normalize(piece):
        def some_lanes(k):
            lanes = aligned(piece * (piece_rows // LANES) + k, LANES)
            scale = gain[lanes].reshape(1, LANES)
            for at in range(row_blocks):
                part = slice(at * LANES, (at + 1) * LANES)
                value = standardized(part, lanes) * scale
                normed_t[0, lanes, part] = value.T.astype(jnp.bfloat16)

        loop(piece_rows // LANES, some_lanes)
        share_normed(aligned(piece, piece_rows)).start()

    loop(pieces, normalize)

    share_query(slice(None)).wait_recv()
    share_normed(slice(None)).wait_recv()

    def contribution(part, to_chip):
        def half(which):
            return jnp.dot(
                normed_t[which, part, :],
                grad_query[to_chip, which * tokens : (which + 1) * tokens, :],
                preferred_element_type=jnp.float32,
            )

        return half(0) + half(1)

    group = blocks // pieces
    last_weight = jnp.maximum(chip, chips - 1 - chip) - 1

    def weight_product(from_chip, weight, piece, first):
        def some_rows(k):
            at = piece * group + k
            value = lax.dot_general(
                grad_query[from_chip],
                weight[aligned(at, block), :],
                (((1,), (1,)), ((), ())),
                preferred_element_type=jnp.float32,
            )
            if first:
                product[at] = value
            else:
                product[at] += value

        loop(group, some_rows)

    def share_product(which, index=0):
        theirs = product.at[which, pl.ds(tokens, tokens)]
        return share(theirs, product_in.at[which], product_sem, index)

    def give(slot, piece):
        def one(way):
            @pl.when(place(way)[1])
            def _():
                hop(way, slot + 1, piece, slots.at[way, slot]).start()

        loop(2, one)

    def slot_step(slot):
        def piece_step(piece):
            part = aligned(piece, piece_rows)

            def take(way):
                behind, ahead = place(way)

                @pl.when(behind > 0)
                def _():
                    arrival(way, slot, piece).wait_recv()

                @pl.when(ahead & (slot >= behind))
                def _():
                    skip = slot - behind
                    to_chip = jnp.where(way == 0, chips - 1 - skip, skip)
                    own = contribution(part, to_chip)

                    @pl.when(behind > 0)
                    def _():
                        held = slots[way, slot, part, :].astype(jnp.float32)
                        slots[way, slot, part, :] = (held + own).astype(jnp.bfloat16)

                    @pl.when(behind == 0)
                    def _():
                        slots[way, slot, part, :] = own.astype(jnp.bfloat16)

            loop(2, take)

            @pl.when((slot < chips - 2) | (piece < pieces - 1))
            def _():
                give(slot, piece)

            @pl.when(slot == 0)
            def _():
                weight_product(chip, w, piece, True)
                own_grad[part, :] = contribution(part, chip)

            def use_weight(way):
                behind, _ = place(way)

                @pl.when(slot < behind)
                def _():
                    from_chip = jnp.where(way == 0, chip - 1 - slot, chip + 1 + slot)
                    weight_product(from_chip, slots.at[way, slot], piece, False)

            loop(2, use_weight)

            @pl.when(slot == last_weight)
            def _():
                share_product(aligned(piece, group), piece).start()

        loop(pieces, piece_step)

    loop(chips - 1, slot_step)

    gain_rows = rows // LANES
    half_rows = gain_parts.shape[1]
    slopes[...] = jnp.zeros_like(slopes)
    per_block = block // LANES

    def slope_sums(at):
        for k in range(per_block):
            inner = slice(k * LANES, (k + 1) * LANES)
            lanes = aligned(at * per_block + k, LANES)
            scale = gain[lanes].reshape(1, LANES)

            def some_rows(row, gain_total):
                part = aligned(row, LANES)
                value = product[at, part, inner] + product_in[at, part, inner]
                product[at, part, inner] = value
                xhat = standardized(part, lanes)
                slope = value * scale
                slopes[0, part, :] += slope
                slopes[1, part, :] += slope * xhat
                return gain_total + jnp.sum((value * xhat).reshape(-1, 8, LANES), axis=0)

            gain_total = lax.fori_loop(0, row_blocks, some_rows, jnp.zeros((8, LANES), jnp.float32))
            gain_parts[(at * per_block + k) // half_rows, pl.ds((at * per_block + k) % half_rows, 1), :] = jnp.sum(gain_total, axis=0, keepdims=True)

    for k in range(pieces):
        share_product(pl.ds(k * group, group), k).wait_recv()
        loop(group, lambda at: slope_sums(k * group + at))

    for at in range(gain_rows, CORES * half_rows):
        total = jnp.sum(qk_part[...], axis=0, keepdims=True)
        row = total if at == gain_rows else jnp.zeros_like(total)
        gain_parts[at // half_rows, at % half_rows : at % half_rows + 1, :] = row

    def spread_gains(k):
        mine = gain_chips.at[chip]
        return pltpu.make_async_remote_copy(
            src_ref=mine,
            dst_ref=mine,
            send_sem=gain_sem.at[0],
            recv_sem=gain_sem.at[1],
            device_id=(lax.rem(dp + CORES * k, dp_count), mp),
            device_id_type=MESH,
        )

    first_swap = share(gain_parts.at[1 - core], gain_in, gain_sem, 1)
    first_swap.start()
    for at in range(row_blocks):
        part = slice(at * LANES, (at + 1) * LANES)
        row_sums[1, 0, at : at + 1, :] = as_row(slopes[0, part, :])
        row_sums[1, 0, row_blocks + at : row_blocks + at + 1, :] = as_row(slopes[1, part, :])
    exchange(1, 0).start()
    first_swap.wait()
    gain_chips[chip] = gain_parts[core] + gain_in[...]
    loop(chips - 1, lambda k: spread_gains(k + 1).start())
    for way in range(2):
        @pl.when(place(way)[1] & (core == 0))
        def _():
            final_hop(way).start()

    for stage in range(stages - 1):
        add_stage(1, stage)
    sums = add_stage(1, stages - 1)
    for at in range(row_blocks):
        part = slice(at * LANES, (at + 1) * LANES)
        slopes[0, part, :] = as_tile(sums[at : at + 1])
        slopes[1, part, :] = as_tile(sums[row_blocks + at : row_blocks + at + 1])

    def finish_rows(row):
        part = aligned(row, LANES)
        for k in range(gain_rows):
            lanes = slice(k * LANES, (k + 1) * LANES)
            at, inner = k // per_block, k % per_block * LANES
            slope = product[at, part, inner : inner + LANES] * gain[lanes].reshape(1, LANES)
            value = deviation[part, :] * (
                slope - slopes[0, part, :] - standardized(part, lanes) * slopes[1, part, :]
            )
            input_grad[part, lanes] = value.astype(jnp.bfloat16)

    loop(row_blocks, finish_rows)

    def own_part(way):
        return slots.at[way, chips - 1, pl.ds(0, (pieces - 1) * piece_rows)]

    def piece_sent(way):
        source = slots.at[way, chips - 1, pl.ds(0, piece_rows)]
        pltpu.make_async_copy(source, source, send_sem.at[2, way]).wait()

    for way in range(2):
        @pl.when(place(way)[1] & (core == 1))
        def _():
            piece_sent(way)
            final_hop(way).start()


    others = gain_chips.at[pl.ds(0, chips - 1)]
    for k in range(2):
        pltpu.make_async_copy(others, others, gain_sem.at[k]).wait()
    gain_totals[core] = lax.fori_loop(1, chips, lambda k, total: total + gain_chips[k], gain_chips[0])
    total = gain_totals.at[core]
    last_swap = share(total, total, gain_sem, 2)
    last_swap.start()
    last_swap.wait()
    for k in range(gain_rows):
        gain_out[k * LANES : (k + 1) * LANES] = gain_totals[k // half_rows, k % half_rows]
    qk_out[...] = gain_totals[gain_rows // half_rows, gain_rows % half_rows]

    def finish_piece(piece):
        part = aligned(piece, piece_rows)

        def one(way):
            @pl.when(place(way)[0] > 0)
            def _():
                arrival(way, chips - 1, piece).wait_recv()
                own_grad[part, :] += slots[way, chips - 1, part, :].astype(jnp.float32)

        loop(2, one)

    share_query(slice(None)).wait_send()
    share_normed(slice(None)).wait_send()
    share_product(slice(None)).wait_send()
    loop(pieces - 1, finish_piece)
    for way in range(2):
        @pl.when(place(way)[0] > 0)
        def _():
            final_hop(way).wait_recv()

    for way in range(2):
        @pl.when(place(way)[1])
        def _():
            @pl.when(core == 0)
            def _():
                piece_sent(way)

            for queue, part in enumerate((slots.at[way, pl.ds(0, chips - 1)], own_part(way))):
                pltpu.make_async_copy(part, part, send_sem.at[queue, way]).wait()


def write_kernel(input_grad, own_grad, tail, gain, qk, input_ref, weight_ref, gain_ref, qk_ref, last, sem):
    rows = own_grad.shape[0]
    most = rows - last.shape[0]
    copies = [
        pltpu.make_async_copy(own_grad.at[pl.ds(0, most)], weight_ref.at[pl.ds(0, most)], sem.at[0]),
        pltpu.make_async_copy(input_grad, input_ref, sem.at[1]),
        pltpu.make_async_copy(gain, gain_ref, sem.at[2]),
        pltpu.make_async_copy(qk, qk_ref, sem.at[3]),
        pltpu.make_async_copy(last, weight_ref.at[pl.ds(most, rows - most)], sem.at[4]),
    ]
    for copy in copies[:-1]:
        copy.start()
    chips = lax.axis_size("dp") // CORES
    chip = lax.axis_index("dp") // CORES
    last[...] = own_grad[most:, :]
    for way, receives in enumerate((chip > 0, chip < chips - 1)):
        @pl.when(receives)
        def _():
            last[...] += tail[way].astype(jnp.float32)

    copies[-1].start()
    for copy in copies:
        copy.wait()


def fused(block_input, prenorm_gain, weight, query, grad_normed, qk_gain):
    dp_count, mp_count = lax.axis_size("dp"), lax.axis_size("mp")
    chips = dp_count // CORES
    tokens, rows = block_input.shape
    columns = weight.shape[1]
    features = query.shape[1]
    pieces = next(count for count in (3, 2) if rows // LANES % count == 0)
    block = math.gcd(rows // pieces, 2 * LANES)
    gain_rows = -(-(rows // LANES + 1) // (8 * CORES)) * 8
    stages = mp_count.bit_length() - 1
    anywhere = pl.BlockSpec(memory_space=pl.ANY)
    local = pl.BlockSpec(memory_space=pltpu.VMEM)
    bf16, f32 = jnp.bfloat16, jnp.float32
    dma = pltpu.SemaphoreType.DMA
    results = pl.pallas_call(
        functools.partial(fused_kernel, (dp_count, mp_count, pieces)),
        in_specs=[anywhere] * 6,
        out_specs=[local] * 5,
        out_shape=[
            pltpu.VMEM((tokens, rows), bf16),
            pltpu.VMEM((rows, columns), f32),
            pltpu.VMEM((2, rows // pieces, columns), bf16),
            pltpu.VMEM((rows,), f32),
            pltpu.VMEM((LANES,), f32),
        ],
        scratch_shapes=[
            pltpu.VMEM((tokens, rows), bf16),
            pltpu.VMEM((rows, columns), bf16),
            pltpu.VMEM((2, tokens, features), bf16),
            pltpu.VMEM((rows,), f32),
            pltpu.VMEM((LANES,), f32),
            pltpu.VMEM((2, chips, rows, columns), bf16),
            pltpu.VMEM((chips, CORES * tokens, columns), bf16),
            pltpu.VMEM((chips, tokens, columns), bf16),
            pltpu.VMEM((CORES, rows, tokens), bf16),
            pltpu.VMEM((rows // block, CORES * tokens, block), f32),
            pltpu.VMEM((rows // block, tokens, block), f32),
            pltpu.VMEM((tokens, LANES), f32),
            pltpu.VMEM((tokens, LANES), f32),
            pltpu.VMEM((2, tokens, LANES), f32),
            pltpu.VMEM((2, stages, 2 * tokens // LANES, LANES), f32),
            pltpu.VMEM((2, stages, 2 * tokens // LANES, LANES), f32),
            pltpu.VMEM((CORES, gain_rows, LANES), f32),
            pltpu.VMEM((gain_rows, LANES), f32),
            pltpu.VMEM((chips, gain_rows, LANES), f32),
            pltpu.VMEM((CORES, gain_rows, LANES), f32),
            pltpu.VMEM((8, LANES), f32),
            dma((4,)),
            dma((pieces,)),
            pltpu.SemaphoreType.REGULAR((2,)),
            dma((3, 2)),
            dma((2, chips, pieces)),
            dma((2,)),
            dma((2,)),
            dma((1 + pieces,)),
            dma((1 + 2 * stages,)),
            dma((4,)),
        ],
        compiler_params=pltpu.CompilerParams(
            collective_id=0, has_side_effects=True, vmem_limit_bytes=56 * 1024 * 1024
        ),
        cost_estimate=pl.CostEstimate(
            flops=8 * tokens * rows * features, bytes_accessed=8 * tokens * features, transcendentals=0
        ),
    )(block_input, prenorm_gain, weight, query, grad_normed, qk_gain)
    outputs = [results[0], results[1], results[3], results[4]]
    return pl.pallas_call(
        write_kernel,
        in_specs=[local] * 5,
        out_specs=[anywhere] * 4,
        out_shape=[jax.ShapeDtypeStruct(output.shape, output.dtype) for output in outputs],
        scratch_shapes=[pltpu.VMEM((rows // pieces, columns), f32), dma((5,))],
        compiler_params=pltpu.CompilerParams(vmem_limit_bytes=4 * 1024 * 1024),
    )(*[pltpu.with_memory_space_constraint(result, pltpu.VMEM) for result in results])


def shards(block_input, prenorm_gain, weight, query, grad_normed, qk_gain):
    tokens, rows = block_input.shape
    sizes = (tokens, rows, weight.shape[1])
    whole_tiles = all(size % LANES == 0 for size in sizes) and qk_gain.shape[0] == LANES
    split = any(rows % (count * LANES) == 0 for count in (2, 3))
    mp_count = lax.axis_size("mp")
    several = lax.axis_size("dp") > CORES and mp_count > 1 and mp_count & (mp_count - 1) == 0
    body = fused if whole_tiles and split and several else permuted
    return body(block_input, prenorm_gain, weight, query, grad_normed, qk_gain)


def solution(mesh):
    return jax.shard_map(
        shards,
        mesh=mesh,
        in_specs=(P("dp", "mp"), P("mp"), P("mp", "dp"), P("dp", None), P("dp", None), P()),
        out_specs=(P("dp", "mp"), P("mp", "dp"), P("mp"), P()),
        check_vma=False,
    )
```

```python
import functools
import math

import jax
import jax.numpy as jnp
from jax import lax
from jax.experimental import pallas as pl
from jax.experimental.pallas import tpu as pltpu
from jax.sharding import PartitionSpec as P

D = 6144


EPS = 1e-06


def qk_kernel(query_ref, grad_ref, gain_ref, out_ref, contrib_ref):
    @pl.when(pl.program_id(0) == 0)
    def _():
        contrib_ref[...] = jnp.zeros_like(contrib_ref)

    head_size = gain_ref.shape[1]
    gain = gain_ref[...]
    total = jnp.zeros_like(contrib_ref)
    for head in range(query_ref.shape[1] // head_size):
        columns = pl.ds(head * head_size, head_size)
        q_float = query_ref[:, columns].astype(jnp.float32)
        upstream = grad_ref[:, columns].astype(jnp.float32)
        q_mean = jnp.mean(q_float, axis=1, keepdims=True)
        q_var = jnp.mean(q_float * q_float, axis=1, keepdims=True) - q_mean * q_mean
        q_inv = lax.rsqrt(q_var + EPS)
        qhat = (q_float - q_mean) * q_inv
        dqhat = upstream * gain
        dq_mean = jnp.mean(dqhat, axis=1, keepdims=True)
        dq_cross = jnp.mean(dqhat * qhat, axis=1, keepdims=True)
        out_ref[:, columns] = (q_inv * (dqhat - dq_mean - qhat * dq_cross)).astype(out_ref.dtype)
        product = upstream * qhat
        total += jnp.sum(product.reshape(-1, 8, head_size), axis=0)
    contrib_ref[...] += total


def qk_backward(query, grad_normed, qk_gain):
    rows, width = query.shape
    head_size = qk_gain.shape[0]
    block = min(rows, 64)
    grad_query, contrib = pl.pallas_call(
        qk_kernel,
        grid=(rows // block,),
        in_specs=[
            pl.BlockSpec((block, width), lambda i: (i, 0)),
            pl.BlockSpec((block, width), lambda i: (i, 0)),
            pl.BlockSpec((1, head_size), lambda i: (0, 0)),
        ],
        out_specs=[
            pl.BlockSpec((block, width), lambda i: (i, 0)),
            pl.BlockSpec((8, head_size), lambda i: (0, 0)),
        ],
        out_shape=[
            jax.ShapeDtypeStruct((rows, width), jnp.bfloat16),
            jax.ShapeDtypeStruct((8, head_size), jnp.float32),
        ],
        compiler_params=pltpu.CompilerParams(vmem_limit_bytes=32 * 1024 * 1024),
        cost_estimate=pl.CostEstimate(flops=40 * rows * width, bytes_accessed=6 * rows * width, transcendentals=0),
    )(query, grad_normed, qk_gain.reshape(1, -1))
    return grad_query, jnp.sum(contrib, axis=0)


CORES = 2


def line_move(value, shift, valid):
    chips = lax.axis_size("dp") // CORES
    pairs = [
        (chip * CORES + core, (chip + shift) * CORES + core)
        for chip in range(chips)
        for core in range(CORES)
        if 0 <= chip + shift < chips and valid(chip)
    ]
    return lax.ppermute(value, "dp", pairs)


def partner_swap(value):
    count = lax.axis_size("dp")
    pairs = [(at, at - at % CORES + (at + 1) % CORES) for at in range(count)]
    return lax.ppermute(value, "dp", pairs)


def add_kernel(*refs):
    total = refs[0][...]
    for ref in refs[1:-1]:
        total = total + ref[...].astype(jnp.float32)
    refs[-1][...] = total.astype(jnp.bfloat16)


def add_terms(*terms):
    rows, width = terms[0].shape
    block = math.gcd(rows, 256)
    spec = pl.BlockSpec((block, width), lambda i: (i, 0))
    return pl.pallas_call(
        add_kernel,
        grid=(rows // block,),
        in_specs=[spec] * len(terms),
        out_specs=spec,
        out_shape=jax.ShapeDtypeStruct((rows, width), jnp.bfloat16),
        compiler_params=pltpu.CompilerParams(vmem_limit_bytes=16 * 1024 * 1024),
        cost_estimate=pl.CostEstimate(
            flops=3 * rows * width, bytes_accessed=10 * rows * width, transcendentals=0
        ),
    )(*terms)


def permuted(block_input, prenorm_gain, weight, query, grad_normed, qk_gain):
    chips = lax.axis_size("dp") // CORES
    chip = lax.axis_index("dp") // CORES
    core = lax.axis_index("dp") % CORES
    columns = weight.shape[1]
    pair_columns = columns * CORES

    steps = []
    rightward, leftward = weight, weight
    for step in range(1, chips):
        rightward = line_move(rightward, 1, lambda at: at - step + 1 >= 0)
        leftward = line_move(leftward, -1, lambda at: at + step - 1 < chips)
        steps.append((rightward, leftward))

    input_wide_float = block_input.astype(jnp.float32)
    local_sum = jnp.sum(input_wide_float, axis=1)
    local_square = jnp.sum(input_wide_float * input_wide_float, axis=1)
    total_sum, total_square = lax.psum((local_sum, local_square), "mp")
    row_average = (total_sum / D)[:, None]
    reciprocal_deviation = lax.rsqrt((total_square / D)[:, None] - row_average * row_average + EPS)
    standardized_input = (input_wide_float - row_average) * reciprocal_deviation
    prenormed_rows = (standardized_input * prenorm_gain).astype(jnp.bfloat16)
    grad_query, qk_partial = qk_backward(query, grad_normed, qk_gain)

    def chip_columns(offset):
        first = lax.rem(chip + offset + chips, chips) * pair_columns
        return lax.dynamic_slice_in_dim(grad_query, first, pair_columns, 1)

    order = []
    for step in range(1, chips):
        for offset in ((chips - step) % chips, step):
            if offset not in order:
                order.append(offset)
    order.append(0)
    own, theirs = {}, {}
    for offset in order:
        part = lax.dot_general(
            prenormed_rows,
            chip_columns(offset),
            (((0,), (0,)), ((), ())),
            preferred_element_type=jnp.float32,
        )
        own[offset] = lax.dynamic_slice_in_dim(part, core * columns, columns, 1)
        theirs[offset] = partner_swap(
            lax.dynamic_slice_in_dim(part, (1 - core) * columns, columns, 1).astype(jnp.bfloat16)
        )

    to_right, to_left = None, None
    for step in range(1, chips):
        right_terms = [own[chips - step], theirs[chips - step]]
        left_terms = [own[step], theirs[step]]
        if step > 1:
            right_terms.append(to_right)
            left_terms.append(to_left)
        to_right = line_move(add_terms(*right_terms), 1, lambda at: at < step)
        to_left = line_move(add_terms(*left_terms), -1, lambda at: at >= chips - step)
    grad_weight = own[0] + theirs[0].astype(jnp.float32)
    if chips > 1:
        grad_weight = grad_weight + to_right.astype(jnp.float32) + to_left.astype(jnp.float32)

    def product(block, offset):
        other = partner_swap(block)
        first = jnp.where(core == 0, block, other)
        second = jnp.where(core == 0, other, block)
        return lax.dot_general(
            chip_columns(offset),
            jnp.concatenate([first, second], axis=1),
            (((1,), (1,)), ((), ())),
            preferred_element_type=jnp.float32,
        )

    gradient_prenormed_input = product(weight, 0)
    for step in range(1, chips):
        rightward, leftward = steps[step - 1]
        if 2 * step >= chips:
            from_left = chip >= step
            gradient_prenormed_input += product(
                jnp.where(from_left, rightward, leftward), jnp.where(from_left, -step, step)
            )
        else:
            gradient_prenormed_input += product(rightward, -step)
            gradient_prenormed_input += product(leftward, step)

    standardized_gradient = gradient_prenormed_input * prenorm_gain
    slope_mean, slope_cross = lax.psum(
        (
            jnp.sum(standardized_gradient, axis=1),
            jnp.sum(standardized_gradient * standardized_input, axis=1),
        ),
        "mp",
    )
    average_standardized_gradient = (slope_mean / D)[:, None]
    average_cross_term = (slope_cross / D)[:, None]
    input_gradient = (
        reciprocal_deviation
        * (
            standardized_gradient
            - average_standardized_gradient
            - standardized_input * average_cross_term
        )
    ).astype(jnp.bfloat16)
    prenorm_gain_partial = jnp.sum(gradient_prenormed_input * standardized_input, axis=0)
    prenorm_gain_gradient, grad_qk_gain = lax.psum((prenorm_gain_partial, qk_partial), "dp")
    return (input_gradient, grad_weight, prenorm_gain_gradient, grad_qk_gain)


LANES = 128
MESH = pl.DeviceIdType.MESH


def loop(count, body):
    def step(i, carry):
        body(i)
        return carry

    lax.fori_loop(0, count, step, 0)


def aligned(at, size):
    return pl.ds(pl.multiple_of(at * size, size), size)


def fused_kernel(
    sizes,
    x_ref,
    gain_ref,
    w_ref,
    query_ref,
    grad_ref,
    qk_gain_ref,
    input_grad,
    own_grad,
    tail,
    gain_out,
    qk_out,
    x,
    w,
    queries,
    gain,
    qk_scale,
    slots,
    grad_query,
    grad_query_out,
    normed_t,
    product,
    product_in,
    average,
    deviation,
    slopes,
    row_sums,
    row_sums_in,
    gain_parts,
    gain_in,
    gain_chips,
    gain_totals,
    qk_part,
    load_sem,
    weight_sem,
    ready_sem,
    send_sem,
    recv_sem,
    query_sem,
    normed_sem,
    product_sem,
    sums_sem,
    gain_sem,
):
    dp_count, mp_count, pieces = sizes
    chips = dp_count // CORES
    tokens, rows = x_ref.shape
    columns = w_ref.shape[1]
    piece_rows = rows // pieces
    width = rows * mp_count
    blocks, _, block = product.shape
    row_blocks = tokens // LANES
    heads = columns // LANES

    dp = lax.axis_index("dp")
    mp = lax.axis_index("mp")
    chip = dp // CORES
    core = dp % CORES
    partner = (chip * CORES + 1 - core, mp)

    stages = mp_count.bit_length() - 1

    def mp_peer(stage):
        bit = 1 << stage
        return (dp, mp + bit - 2 * bit * (mp // bit % 2))

    def load_weight(piece):
        part = aligned(piece, piece_rows)
        return pltpu.make_async_copy(w_ref.at[part], w.at[part], weight_sem.at[piece])

    loop(pieces, lambda piece: load_weight(piece).start())

    barrier = pltpu.get_barrier_semaphore()

    def place(way):
        behind = jnp.where(way == 0, chip, chips - 1 - chip)
        return behind, behind < chips - 1

    def next_chip(way):
        return (dp + CORES * (1 - 2 * way), mp)

    def tell(semaphore, peer):
        pl.semaphore_signal(semaphore, inc=1, device_id=peer, device_id_type=MESH)

    pairs = [(chip > 0, next_chip(1), chip < chips - 1, next_chip(0)), (core == 1, partner, core == 0, partner)]
    for stage in range(stages):
        low = mp // (1 << stage) % 2 == 0
        pairs.append((~low, mp_peer(stage), low, mp_peer(stage)))
    for _, _, below, peer in pairs:
        @pl.when(below)
        def _():
            tell(barrier, peer)

    above_count = sum(jnp.where(above, 1, 0) for above, _, _, _ in pairs)

    @pl.when(above_count > 0)
    def _():
        pl.semaphore_wait(barrier, above_count)

    for k, (above, peer, _, _) in enumerate(pairs):
        @pl.when(above)
        def _():
            tell(ready_sem.at[min(k, 1)], peer)

    def await_ready(group, which):
        count = sum(jnp.where(below, 1, 0) for _, _, below, _ in which)

        @pl.when(count > 0)
        def _():
            pl.semaphore_wait(ready_sem.at[group], count)

    def queue_of(slot, piece):
        late = jnp.where(slot == chips - 1, 1, 0)
        return late + late * jnp.where(piece == pieces - 2, 1, 0)

    def hop(way, slot, piece, source):
        part = aligned(piece, piece_rows)
        return pltpu.make_async_remote_copy(
            src_ref=source.at[part],
            dst_ref=slots.at[way, slot, part],
            send_sem=send_sem.at[queue_of(slot, piece), way],
            recv_sem=recv_sem.at[way, slot, piece],
            device_id=next_chip(way),
            device_id_type=MESH,
        )

    def final_hop(way):
        part = pl.ds((pieces - 1) * piece_rows, piece_rows)
        return pltpu.make_async_remote_copy(
            src_ref=slots.at[way, chips - 2, part],
            dst_ref=tail.at[way],
            send_sem=send_sem.at[1, way],
            recv_sem=recv_sem.at[way, chips - 1, pieces - 1],
            device_id=next_chip(way),
            device_id_type=MESH,
        )

    def arrival(way, slot, piece):
        return hop(way, slot, piece, slots.at[way, slot])

    def send_weight(piece, way):
        @pl.when(place(way)[1])
        def _():
            hop(way, 0, piece, w).start()

    def load_and_send(piece):
        load_weight(piece).wait()
        send_weight(piece, 1)

    loop(pieces, load_and_send)
    await_ready(0, pairs[:1])
    loop(pieces, lambda piece: send_weight(piece, 0))

    loads = [
        pltpu.make_async_copy(source, target, load_sem.at[i])
        for i, (source, target) in enumerate(
            ((x_ref, x), (gain_ref, gain), (qk_gain_ref, qk_scale))
        )
    ]
    for load in loads:
        load.start()
    for k, source in enumerate((query_ref, grad_ref)):
        pltpu.make_async_copy(source, queries.at[k], load_sem.at[3]).start()

    def exchange(kind, stage):
        return pltpu.make_async_remote_copy(
            src_ref=row_sums.at[kind, stage],
            dst_ref=row_sums_in.at[kind, stage],
            send_sem=sums_sem.at[0],
            recv_sem=sums_sem.at[1 + kind * stages + stage],
            device_id=mp_peer(stage),
            device_id_type=MESH,
        )

    def add_stage(kind, stage):
        exchange(kind, stage).wait()
        total = row_sums[kind, stage] + row_sums_in[kind, stage]
        if stage + 1 == stages:
            return total * (1.0 / width)
        row_sums[kind, stage + 1] = total
        exchange(kind, stage + 1).start()

    diagonal = lax.broadcasted_iota(jnp.int32, (LANES, LANES), 0) == lax.broadcasted_iota(
        jnp.int32, (LANES, LANES), 1
    )

    def as_row(tile):
        total = jnp.sum(tile, axis=1, keepdims=True)
        return jnp.sum(jnp.where(diagonal, total, 0.0), axis=0, keepdims=True)

    def as_tile(row):
        total = jnp.sum(jnp.where(diagonal, row, 0.0), axis=1, keepdims=True)
        return jnp.broadcast_to(total, (LANES, LANES))

    loads[0].wait()

    def input_sums(at):
        part = aligned(at, LANES)
        total = jnp.zeros((LANES, LANES), jnp.float32)
        square = jnp.zeros((LANES, LANES), jnp.float32)
        for k in range(rows // LANES):
            value = x[part, k * LANES : (k + 1) * LANES].astype(jnp.float32)
            total += value
            square += value * value
        row_sums[0, 0, pl.ds(at, 1), :] = as_row(total)
        row_sums[0, 0, pl.ds(row_blocks + at, 1), :] = as_row(square)

    loop(row_blocks, input_sums)
    await_ready(1, pairs[1:])
    exchange(0, 0).start()

    for load in loads[1:]:
        load.wait()
    pltpu.make_async_copy(queries, queries, load_sem.at[3]).wait()
    qk_gain = qk_scale[...].reshape(1, LANES)
    qk_part[...] = jnp.zeros_like(qk_part)
    chunk = 64

    def qk_columns(to_chip, half, target):
        first = (to_chip * CORES + half) * columns

        def some_rows(at):
            part = aligned(at, chunk)
            total = jnp.zeros_like(qk_part)
            for head in range(heads):
                lanes = pl.ds(pl.multiple_of(first + head * LANES, LANES), LANES)
                q_float = queries[0, part, lanes].astype(jnp.float32)
                upstream = queries[1, part, lanes].astype(jnp.float32)
                q_mean = jnp.mean(q_float, axis=1, keepdims=True)
                q_var = jnp.mean(q_float * q_float, axis=1, keepdims=True) - q_mean * q_mean
                q_inv = lax.rsqrt(q_var + EPS)
                qhat = (q_float - q_mean) * q_inv
                dqhat = upstream * qk_gain
                dq_mean = jnp.mean(dqhat, axis=1, keepdims=True)
                dq_cross = jnp.mean(dqhat * qhat, axis=1, keepdims=True)
                out = q_inv * (dqhat - dq_mean - qhat * dq_cross)
                target[to_chip, part, head * LANES : (head + 1) * LANES] = out.astype(jnp.bfloat16)
                total += jnp.sum((upstream * qhat).reshape(-1, 8, LANES), axis=0)
            qk_part[...] += total

        loop(tokens // chunk, some_rows)

    def share(source, target, sem, index=0):
        return pltpu.make_async_remote_copy(
            src_ref=source,
            dst_ref=target,
            send_sem=sem.at[0],
            recv_sem=sem.at[1 + index],
            device_id=partner,
            device_id_type=MESH,
        )

    def share_query(which):
        return share(grad_query_out.at[which], grad_query.at[which, pl.ds(tokens, tokens)], query_sem)

    def partner_columns(to_chip):
        qk_columns(to_chip, 1 - core, grad_query_out)
        share_query(to_chip).start()

    loop(chips, partner_columns)
    for stage in range(stages - 1):
        add_stage(0, stage)
    loop(chips, lambda to_chip: qk_columns(to_chip, core, grad_query))

    sums = add_stage(0, stages - 1)
    means = sums[:row_blocks]
    scales = lax.rsqrt(sums[row_blocks:] - means * means + EPS)
    for at in range(row_blocks):
        average[at * LANES : (at + 1) * LANES, :] = as_tile(means[at : at + 1])
        deviation[at * LANES : (at + 1) * LANES, :] = as_tile(scales[at : at + 1])

    def standardized(part, lanes):
        return (x[part, lanes].astype(jnp.float32) - average[part, :]) * deviation[part, :]

    def share_normed(part):
        return share(normed_t.at[0, part], normed_t.at[1, part], normed_sem)

    def normalize(piece):
        def some_lanes(k):
            lanes = aligned(piece * (piece_rows // LANES) + k, LANES)
            scale = gain[lanes].reshape(1, LANES)
            for at in range(row_blocks):
                part = slice(at * LANES, (at + 1) * LANES)
                value = standardized(part, lanes) * scale
                normed_t[0, lanes, part] = value.T.astype(jnp.bfloat16)

        loop(piece_rows // LANES, some_lanes)
        share_normed(aligned(piece, piece_rows)).start()

    loop(pieces, normalize)

    share_query(slice(None)).wait_recv()
    share_normed(slice(None)).wait_recv()

    def contribution(part, to_chip):
        def half(which):
            return jnp.dot(
                normed_t[which, part, :],
                grad_query[to_chip, which * tokens : (which + 1) * tokens, :],
                preferred_element_type=jnp.float32,
            )

        return half(0) + half(1)

    group = blocks // pieces
    last_weight = jnp.maximum(chip, chips - 1 - chip) - 1

    def weight_product(from_chip, weight, piece, first):
        def some_rows(k):
            at = piece * group + k
            value = lax.dot_general(
                grad_query[from_chip],
                weight[aligned(at, block), :],
                (((1,), (1,)), ((), ())),
                preferred_element_type=jnp.float32,
            )
            if first:
                product[at] = value
            else:
                product[at] += value

        loop(group, some_rows)

    def share_product(which, index=0):
        theirs = product.at[which, pl.ds(tokens, tokens)]
        return share(theirs, product_in.at[which], product_sem, index)

    def give(slot, piece):
        def one(way):
            @pl.when(place(way)[1])
            def _():
                hop(way, slot + 1, piece, slots.at[way, slot]).start()

        loop(2, one)

    def slot_step(slot):
        def piece_step(piece):
            part = aligned(piece, piece_rows)

            def take(way):
                behind, ahead = place(way)

                @pl.when(behind > 0)
                def _():
                    arrival(way, slot, piece).wait_recv()

                @pl.when(ahead & (slot >= behind))
                def _():
                    skip = slot - behind
                    to_chip = jnp.where(way == 0, chips - 1 - skip, skip)
                    own = contribution(part, to_chip)

                    @pl.when(behind > 0)
                    def _():
                        held = slots[way, slot, part, :].astype(jnp.float32)
                        slots[way, slot, part, :] = (held + own).astype(jnp.bfloat16)

                    @pl.when(behind == 0)
                    def _():
                        slots[way, slot, part, :] = own.astype(jnp.bfloat16)

            loop(2, take)

            @pl.when((slot < chips - 2) | (piece < pieces - 1))
            def _():
                give(slot, piece)

            @pl.when(slot == 0)
            def _():
                weight_product(chip, w, piece, True)
                own_grad[part, :] = contribution(part, chip)

            def use_weight(way):
                behind, _ = place(way)

                @pl.when(slot < behind)
                def _():
                    from_chip = jnp.where(way == 0, chip - 1 - slot, chip + 1 + slot)
                    weight_product(from_chip, slots.at[way, slot], piece, False)

            loop(2, use_weight)

            @pl.when(slot == last_weight)
            def _():
                share_product(aligned(piece, group), piece).start()

        loop(pieces, piece_step)

    loop(chips - 1, slot_step)

    gain_rows = rows // LANES
    half_rows = gain_parts.shape[1]
    slopes[...] = jnp.zeros_like(slopes)
    per_block = block // LANES

    def slope_sums(at):
        for k in range(per_block):
            inner = slice(k * LANES, (k + 1) * LANES)
            lanes = aligned(at * per_block + k, LANES)
            scale = gain[lanes].reshape(1, LANES)

            def some_rows(row, gain_total):
                part = aligned(row, LANES)
                value = product[at, part, inner] + product_in[at, part, inner]
                product[at, part, inner] = value
                xhat = standardized(part, lanes)
                slope = value * scale
                slopes[0, part, :] += slope
                slopes[1, part, :] += slope * xhat
                return gain_total + jnp.sum((value * xhat).reshape(-1, 8, LANES), axis=0)

            gain_total = lax.fori_loop(0, row_blocks, some_rows, jnp.zeros((8, LANES), jnp.float32))
            gain_parts[(at * per_block + k) // half_rows, pl.ds((at * per_block + k) % half_rows, 1), :] = jnp.sum(gain_total, axis=0, keepdims=True)

    for k in range(pieces):
        share_product(pl.ds(k * group, group), k).wait_recv()
        loop(group, lambda at: slope_sums(k * group + at))

    for at in range(gain_rows, CORES * half_rows):
        total = jnp.sum(qk_part[...], axis=0, keepdims=True)
        row = total if at == gain_rows else jnp.zeros_like(total)
        gain_parts[at // half_rows, at % half_rows : at % half_rows + 1, :] = row

    def spread_gains(k):
        mine = gain_chips.at[chip]
        return pltpu.make_async_remote_copy(
            src_ref=mine,
            dst_ref=mine,
            send_sem=gain_sem.at[0],
            recv_sem=gain_sem.at[1],
            device_id=(lax.rem(dp + CORES * k, dp_count), mp),
            device_id_type=MESH,
        )

    first_swap = share(gain_parts.at[1 - core], gain_in, gain_sem, 1)
    first_swap.start()
    for at in range(row_blocks):
        part = slice(at * LANES, (at + 1) * LANES)
        row_sums[1, 0, at : at + 1, :] = as_row(slopes[0, part, :])
        row_sums[1, 0, row_blocks + at : row_blocks + at + 1, :] = as_row(slopes[1, part, :])
    exchange(1, 0).start()
    first_swap.wait()
    gain_chips[chip] = gain_parts[core] + gain_in[...]
    loop(chips - 1, lambda k: spread_gains(k + 1).start())
    for way in range(2):
        @pl.when(place(way)[1] & (core == 0))
        def _():
            final_hop(way).start()

    for stage in range(stages - 1):
        add_stage(1, stage)
    sums = add_stage(1, stages - 1)
    for at in range(row_blocks):
        part = slice(at * LANES, (at + 1) * LANES)
        slopes[0, part, :] = as_tile(sums[at : at + 1])
        slopes[1, part, :] = as_tile(sums[row_blocks + at : row_blocks + at + 1])

    def finish_rows(row):
        part = aligned(row, LANES)
        for k in range(gain_rows):
            lanes = slice(k * LANES, (k + 1) * LANES)
            at, inner = k // per_block, k % per_block * LANES
            slope = product[at, part, inner : inner + LANES] * gain[lanes].reshape(1, LANES)
            value = deviation[part, :] * (
                slope - slopes[0, part, :] - standardized(part, lanes) * slopes[1, part, :]
            )
            input_grad[part, lanes] = value.astype(jnp.bfloat16)

    loop(row_blocks, finish_rows)

    def own_part(way):
        return slots.at[way, chips - 1, pl.ds(0, (pieces - 1) * piece_rows)]

    def piece_sent(way):
        source = slots.at[way, chips - 1, pl.ds(0, piece_rows)]
        pltpu.make_async_copy(source, source, send_sem.at[2, way]).wait()

    for way in range(2):
        @pl.when(place(way)[1] & (core == 1))
        def _():
            piece_sent(way)
            final_hop(way).start()


    others = gain_chips.at[pl.ds(0, chips - 1)]
    for k in range(2):
        pltpu.make_async_copy(others, others, gain_sem.at[k]).wait()
    gain_totals[core] = lax.fori_loop(1, chips, lambda k, total: total + gain_chips[k], gain_chips[0])
    total = gain_totals.at[core]
    last_swap = share(total, total, gain_sem, 2)
    last_swap.start()
    last_swap.wait()
    for k in range(gain_rows):
        gain_out[k * LANES : (k + 1) * LANES] = gain_totals[k // half_rows, k % half_rows]
    qk_out[...] = gain_totals[gain_rows // half_rows, gain_rows % half_rows]

    def finish_piece(piece):
        part = aligned(piece, piece_rows)

        def one(way):
            @pl.when(place(way)[0] > 0)
            def _():
                arrival(way, chips - 1, piece).wait_recv()
                own_grad[part, :] += slots[way, chips - 1, part, :].astype(jnp.float32)

        loop(2, one)

    share_query(slice(None)).wait_send()
    share_normed(slice(None)).wait_send()
    share_product(slice(None)).wait_send()
    loop(pieces - 1, finish_piece)
    for way in range(2):
        @pl.when(place(way)[0] > 0)
        def _():
            final_hop(way).wait_recv()

    for way in range(2):
        @pl.when(place(way)[1])
        def _():
            @pl.when(core == 0)
            def _():
                piece_sent(way)

            for queue, part in enumerate((slots.at[way, pl.ds(0, chips - 1)], own_part(way))):
                pltpu.make_async_copy(part, part, send_sem.at[queue, way]).wait()


def write_kernel(input_grad, own_grad, tail, gain, qk, input_ref, weight_ref, gain_ref, qk_ref, last, sem):
    rows = own_grad.shape[0]
    most = rows - last.shape[0]
    copies = [
        pltpu.make_async_copy(own_grad.at[pl.ds(0, most)], weight_ref.at[pl.ds(0, most)], sem.at[0]),
        pltpu.make_async_copy(input_grad, input_ref, sem.at[1]),
        pltpu.make_async_copy(gain, gain_ref, sem.at[2]),
        pltpu.make_async_copy(qk, qk_ref, sem.at[3]),
        pltpu.make_async_copy(last, weight_ref.at[pl.ds(most, rows - most)], sem.at[4]),
    ]
    for copy in copies[:-1]:
        copy.start()
    chips = lax.axis_size("dp") // CORES
    chip = lax.axis_index("dp") // CORES
    last[...] = own_grad[most:, :]
    for way, receives in enumerate((chip > 0, chip < chips - 1)):
        @pl.when(receives)
        def _():
            last[...] += tail[way].astype(jnp.float32)

    copies[-1].start()
    for copy in copies:
        copy.wait()


def fused(block_input, prenorm_gain, weight, query, grad_normed, qk_gain):
    dp_count, mp_count = lax.axis_size("dp"), lax.axis_size("mp")
    chips = dp_count // CORES
    tokens, rows = block_input.shape
    columns = weight.shape[1]
    features = query.shape[1]
    pieces = next(count for count in (2, 3) if rows // LANES % count == 0)
    block = math.gcd(rows // pieces, 2 * LANES)
    gain_rows = -(-(rows // LANES + 1) // (8 * CORES)) * 8
    stages = mp_count.bit_length() - 1
    anywhere = pl.BlockSpec(memory_space=pl.ANY)
    local = pl.BlockSpec(memory_space=pltpu.VMEM)
    bf16, f32 = jnp.bfloat16, jnp.float32
    dma = pltpu.SemaphoreType.DMA
    results = pl.pallas_call(
        functools.partial(fused_kernel, (dp_count, mp_count, pieces)),
        in_specs=[anywhere] * 6,
        out_specs=[local] * 5,
        out_shape=[
            pltpu.VMEM((tokens, rows), bf16),
            pltpu.VMEM((rows, columns), f32),
            pltpu.VMEM((2, rows // pieces, columns), bf16),
            pltpu.VMEM((rows,), f32),
            pltpu.VMEM((LANES,), f32),
        ],
        scratch_shapes=[
            pltpu.VMEM((tokens, rows), bf16),
            pltpu.VMEM((rows, columns), bf16),
            pltpu.VMEM((2, tokens, features), bf16),
            pltpu.VMEM((rows,), f32),
            pltpu.VMEM((LANES,), f32),
            pltpu.VMEM((2, chips, rows, columns), bf16),
            pltpu.VMEM((chips, CORES * tokens, columns), bf16),
            pltpu.VMEM((chips, tokens, columns), bf16),
            pltpu.VMEM((CORES, rows, tokens), bf16),
            pltpu.VMEM((rows // block, CORES * tokens, block), f32),
            pltpu.VMEM((rows // block, tokens, block), f32),
            pltpu.VMEM((tokens, LANES), f32),
            pltpu.VMEM((tokens, LANES), f32),
            pltpu.VMEM((2, tokens, LANES), f32),
            pltpu.VMEM((2, stages, 2 * tokens // LANES, LANES), f32),
            pltpu.VMEM((2, stages, 2 * tokens // LANES, LANES), f32),
            pltpu.VMEM((CORES, gain_rows, LANES), f32),
            pltpu.VMEM((gain_rows, LANES), f32),
            pltpu.VMEM((chips, gain_rows, LANES), f32),
            pltpu.VMEM((CORES, gain_rows, LANES), f32),
            pltpu.VMEM((8, LANES), f32),
            dma((4,)),
            dma((pieces,)),
            pltpu.SemaphoreType.REGULAR((2,)),
            dma((3, 2)),
            dma((2, chips, pieces)),
            dma((2,)),
            dma((2,)),
            dma((1 + pieces,)),
            dma((1 + 2 * stages,)),
            dma((4,)),
        ],
        compiler_params=pltpu.CompilerParams(
            collective_id=0, has_side_effects=True, vmem_limit_bytes=56 * 1024 * 1024
        ),
        cost_estimate=pl.CostEstimate(
            flops=8 * tokens * rows * features, bytes_accessed=8 * tokens * features, transcendentals=0
        ),
    )(block_input, prenorm_gain, weight, query, grad_normed, qk_gain)
    outputs = [results[0], results[1], results[3], results[4]]
    return pl.pallas_call(
        write_kernel,
        in_specs=[local] * 5,
        out_specs=[anywhere] * 4,
        out_shape=[jax.ShapeDtypeStruct(output.shape, output.dtype) for output in outputs],
        scratch_shapes=[pltpu.VMEM((rows // pieces, columns), f32), dma((5,))],
        compiler_params=pltpu.CompilerParams(vmem_limit_bytes=4 * 1024 * 1024),
    )(*[pltpu.with_memory_space_constraint(result, pltpu.VMEM) for result in results])


def shards(block_input, prenorm_gain, weight, query, grad_normed, qk_gain):
    tokens, rows = block_input.shape
    sizes = (tokens, rows, weight.shape[1])
    whole_tiles = all(size % LANES == 0 for size in sizes) and qk_gain.shape[0] == LANES
    split = any(rows % (count * LANES) == 0 for count in (2, 3))
    mp_count = lax.axis_size("mp")
    several = lax.axis_size("dp") > CORES and mp_count > 1 and mp_count & (mp_count - 1) == 0
    body = fused if whole_tiles and split and several else permuted
    return body(block_input, prenorm_gain, weight, query, grad_normed, qk_gain)


def solution(mesh):
    return jax.shard_map(
        shards,
        mesh=mesh,
        in_specs=(P("dp", "mp"), P("mp"), P("mp", "dp"), P("dp", None), P("dp", None), P()),
        out_specs=(P("dp", "mp"), P("mp", "dp"), P("mp"), P()),
        check_vma=False,
    )
```
